512 devices in a mesh: gx: 32 (over x, z), gy: 8 (over y_lo, core), gz: 2 (over y_hi).
Axes of the slice: x: 4, y: 8 (y_hi: 2, y_lo: 4; y = y_hi * 4 + y_lo), z: 8, core: 2. Of those that a mesh axis runs over, the one named last changes fastest.
Arguments:
- positions: float32 [64, 32, 8, 8, 3], P('gx', 'gy', 'gz'), may hold values from 0 to 1
- species: int32 [64, 32, 8, 8], P('gx', 'gy', 'gz'), may hold values from 0 to 3
- neighbors: int32 [64, 32, 8, 8, 16], P('gx', 'gy', 'gz'), may hold values from 0 to 215, as said below
- edge_mask: int32 [64, 32, 8, 8, 16], P('gx', 'gy', 'gz'), may hold values 0 or 1
- species_embed: float32 [4, 128], replicated, may hold values from -6 to 6
- radial_weight: float32 [2, 8, 384], replicated, may hold values from -6 to 6
- mix_weight: float32 [2, 384, 128], replicated, may hold values from -0.3125 to 0.3125
- readout: float32 [128], replicated, may hold values from -0.5 to 0.5
- energy_offset: float32 [4], replicated, may hold values from -6 to 6
Outputs:
- atom_energy: float32 [64, 32, 8, 8], P('gx', 'gy', 'gz')
- forces: float32 [64, 32, 8, 8, 3], P('gx', 'gy', 'gz')
The draws below stay inside these ranges and needn't reach their ends.
Inputs may be any that keep to these rules, and one draw needn't show every extreme that they name: `neighbors`: each entry lies in 0 to 215 and names slot n mod 8 of the cell at offset (n // 72 - 1, (n // 24) mod 3 - 1, (n // 8) mod 3 - 1), periodic; it never names the receiving atom itself (104 plus its own slot). Repeats may occur.
All inputs are finite; a program needn't handle non-finite values.
Results may differ from the reference program's by a relative error of at most 0.0003.
Values sent between devices are 32-bit elements.
No kernel may reach another device: no remote copies, remote signals or barrier semaphores. Data moves between devices by JAX's collectives and lax.ppermute only.
A program may use at most 128 MiB of HBM per device.

```python
import math
import jax
import jax.numpy as jnp
from jax import lax

K = 8
E = 16
C = 128
NB = 8
S = 4
LAYERS = 2
NX = 64
NY = 32
NZ = 8


def draw_neighbors(key, part):
    arr_shape = (NX, NY, NZ, K, E)
    raw_ids = jax.random.randint(key, arr_shape, 0, 27 * K - 1, dtype=jnp.int32)
    own_slot = 13 * K + lax.broadcasted_iota(jnp.int32, arr_shape, 3)
    return raw_ids + (raw_ids >= own_slot).astype(jnp.int32)


def with_ends(values, rng, smallest, largest):
    shape = values.shape
    spot = [jax.random.randint(jax.random.fold_in(rng, axis), (), 0, shape[axis]) for axis in range(len(shape))]
    values = values.at[tuple(spot)].set(smallest)
    longest = shape.index(max(shape))
    spot[longest] = (spot[longest] + 1) % shape[longest]
    return values.at[tuple(spot)].set(largest)


def block_scale(own_key, extent, pieces, low, top_value):
    factor_of = 1.0
    for dim, parts in pieces:
        draws = jax.random.uniform(jax.random.fold_in(jax.random.fold_in(own_key, 6), dim), (parts,), jnp.float32, low / len(pieces), top_value / len(pieces))
        factor_of = factor_of * jnp.repeat(jnp.exp(draws), extent[dim] // parts).reshape((-1,) + (1,) * (len(extent) - 1 - dim))
    return factor_of


def scatter_about(rng, shape, spread, most, kind=jnp.bfloat16):
    values = jax.random.normal(rng, shape, jnp.float32) * spread
    return jnp.minimum(jnp.maximum(values, -most), most).astype(kind)


def setup_inputs(seed: int = 0) -> dict:
    arg_keys = jax.random.split(jax.random.key(seed), 10)
    return {
        "positions": jnp.clip(1.0 * jax.random.uniform(arg_keys[0], (NX, NY, NZ, K, 3), jnp.float32) ** block_scale(arg_keys[0], (NX, NY, NZ, K, 3), ((0, 32), (1, 8), (2, 2)), -0.2, 0.2), 0.0, 1.0),
        "species": with_ends(jax.random.randint(arg_keys[1], (NX, NY, NZ, K), 0, S), jax.random.fold_in(arg_keys[1], 1), 0, S - 1).astype(jnp.int32),
        "neighbors": draw_neighbors(jax.random.fold_in(arg_keys[9], 71), 0),
        "edge_mask": with_ends((jax.random.randint(arg_keys[3], (NX, NY, NZ, K, E), 0, 4) < 3).astype(jnp.int32), jax.random.fold_in(arg_keys[3], 1), 0, 1),
        "species_embed": scatter_about(arg_keys[4], (S, C), 1.0, 6.0, jnp.float32),
        "radial_weight": scatter_about(arg_keys[5], (LAYERS, NB, 3 * C), 1.0, 6.0, jnp.float32),
        "mix_weight": scatter_about(arg_keys[6], (LAYERS, 3 * C, C), (3 * C) ** -0.5, 0.3125, jnp.float32),
        "readout": scatter_about(arg_keys[7], (C,), C ** -0.5, 0.5, jnp.float32),
        "energy_offset": scatter_about(arg_keys[8], (S,), 1.0, 6.0, jnp.float32),
    }


cutoff_radius = 2.0
highest = lax.Precision.HIGHEST

def stencil_parts(neighbor_ids, slot_count):
    stencil = neighbor_ids // slot_count
    return (stencil // 9 - 1, stencil // 3 % 3 - 1, stencil % 3 - 1, neighbor_ids % slot_count)

def sender_rows(neighbor_ids, grid_y, grid_z, margin):
    arr_shape = neighbor_ids.shape
    slot_count = arr_shape[3]
    step_x, step_y, step_z, slot_id = stencil_parts(neighbor_ids, slot_count)
    cell_x = lax.broadcasted_iota(jnp.int32, arr_shape, 0) + margin + step_x
    cell_y = lax.broadcasted_iota(jnp.int32, arr_shape, 1) + margin + step_y
    cell_z = lax.broadcasted_iota(jnp.int32, arr_shape, 2) + margin + step_z
    return ((cell_x * grid_y + cell_y) * grid_z + cell_z) * slot_count + slot_id

def displacement(pos_padded, pos_own, neighbor_ids, sender_idx):
    step_x, step_y, step_z, slot_id = stencil_parts(neighbor_ids, neighbor_ids.shape[3])
    offsets = jnp.stack([step_x, step_y, step_z], -1).astype(jnp.float32)
    remote = pos_padded.reshape(-1, 3)[sender_idx]
    return offsets + remote - pos_own[..., None, :]

def edge_basis(displace, basis_count):
    radius_sq = lax.optimization_barrier(jnp.sum(displace * displace, -1))
    radius = jnp.sqrt(radius_sq)
    envelope = jnp.where(radius < cutoff_radius, (1.0 - radius_sq / cutoff_radius ** 2) ** 2, 0.0)
    centres = jnp.arange(basis_count, dtype=jnp.float32) * (cutoff_radius / (basis_count - 1))
    sharpness = ((basis_count - 1) / cutoff_radius) ** 2
    radial_basis = jnp.exp(-sharpness * (radius[..., None] - centres) ** 2) * envelope[..., None]
    scaled = displace / cutoff_radius
    along_x = scaled[..., 0]
    along_y = scaled[..., 1]
    along_z = scaled[..., 2]
    first_order = math.sqrt(3.0) * scaled
    root_15 = math.sqrt(15.0)
    second_order = jnp.stack([root_15 * along_x * along_y, root_15 * along_y * along_z, 0.5 * math.sqrt(5.0) * (3.0 * along_z * along_z - lax.optimization_barrier(jnp.sum(scaled * scaled, -1))), root_15 * along_x * along_z, 0.5 * root_15 * (along_x * along_x - along_y * along_y)], -1)
    return (radial_basis, first_order, second_order)

def interact(senders, radial_basis, first_order, second_order, edge_mask, radial_w, mix_w):
    channels = senders.shape[-1]
    radial = jnp.einsum('...k,kc->...c', radial_basis, radial_w, precision=highest)
    gate_mask = edge_mask.astype(jnp.float32)[..., None]
    term_zero = gate_mask * radial[..., :channels] * senders
    term_one = gate_mask * radial[..., channels:2 * channels] * senders
    term_two = gate_mask * radial[..., 2 * channels:] * senders
    norm_scale = senders.shape[-2] ** (-0.5)
    scalar_part = norm_scale * lax.optimization_barrier(jnp.sum(term_zero, -2))
    vector_part = norm_scale * jnp.einsum('...em,...ec->...mc', first_order, term_one, precision=highest)
    tensor_part = norm_scale * jnp.einsum('...em,...ec->...mc', second_order, term_two, precision=highest)
    invariants = jnp.concatenate([scalar_part, lax.optimization_barrier(jnp.sum(vector_part * vector_part, -2)), lax.optimization_barrier(jnp.sum(tensor_part * tensor_part, -2))], -1)
    return jax.nn.silu(jnp.einsum('...j,jc->...c', invariants, mix_w, precision=highest))

def pad_cells(values):
    margins = ((1, 1), (1, 1), (1, 1)) + ((0, 0),) * (values.ndim - 3)
    return jnp.pad(values, margins, mode='wrap')

def reference(positions, species, neighbors, edge_mask, species_embed, radial_weight, mix_weight, readout, energy_offset):
    grid_x = neighbors.shape[0]
    grid_y = neighbors.shape[1]
    grid_z = neighbors.shape[2]
    channels = species_embed.shape[1]
    sender_idx = sender_rows(neighbors, grid_y + 2, grid_z + 2, 1)
    start_feat = species_embed[species]

    def energy_of(pos_all):
        displace = displacement(pad_cells(pos_all), pos_all, neighbors, sender_idx)
        hidden = start_feat
        for layer_idx in range(LAYERS):
            feat_table = pad_cells(hidden).reshape(-1, channels)

            def slab_update(slab_idx):
                radial_basis, first_order, second_order = edge_basis(displace[slab_idx], NB)
                return interact(feat_table[sender_idx[slab_idx]], radial_basis, first_order, second_order, edge_mask[slab_idx], radial_weight[layer_idx], mix_weight[layer_idx])
            hidden = hidden + lax.map(jax.checkpoint(slab_update), jnp.arange(grid_x, dtype=jnp.int32))
        return energy_offset[species] + jnp.einsum('...c,c->...', hidden, readout, precision=highest)
    energy, pull_back = jax.vjp(energy_of, positions)
    grad_pos, = pull_back(jnp.ones_like(energy))
    return (energy, -grad_pos)
```

```python
import math

import jax
import jax.numpy as jnp
from jax import lax
from jax.experimental import pallas as pl
from jax.experimental.pallas import tpu as pltpu
from jax.sharding import PartitionSpec as P

f32 = jnp.float32
bf16 = jnp.bfloat16
i32 = jnp.int32

E = 16
C = 128
NB = 8
L = 128
CUT = 2.0
GAMMA = ((NB - 1) / CUT) ** 2
SCALE = E**-0.5
R3 = math.sqrt(3.0)
R5 = math.sqrt(5.0)
R15 = math.sqrt(15.0)
VMEM = pltpu.VMEM
SMEM = pltpu.SMEM


def split2(x):
    high = x.astype(bf16)
    low = (x - high.astype(f32)).astype(bf16)
    return high, low


def split3(x):
    high = x.astype(bf16)
    rest = x - high.astype(f32)
    mid = rest.astype(bf16)
    low = (rest - mid.astype(f32)).astype(bf16)
    return high, mid, low


def dot(a, b, dims=((1,), (0,))):
    return lax.dot_general(a, b, (dims, ((), ())), preferred_element_type=f32)


def iota(shape, dim):
    return lax.broadcasted_iota(i32, shape, dim)


def roll(x, shift):
    return pltpu.roll(x, shift % x.shape[-1], x.ndim - 1)


def lanes(shape):
    return iota(shape, len(shape) - 1)


def pack_kernel(gz_ref, pos_ref, spec_ref, nbr_ref, mask_ref, own_ref, straight_ref, cross_ref):
    eye16 = jnp.where(iota((E, E), 0) == iota((E, E), 1), 1.0, 0.0).astype(bf16)
    own_ref[0:16, :] = dot(eye16, nbr_ref[...].astype(f32).astype(bf16), ((1,), (1,)))
    own_ref[16:32, :] = dot(eye16, mask_ref[...].astype(f32).astype(bf16), ((1,), (1,)))
    eye3 = jnp.where(iota((8, 3), 0) == iota((8, 3), 1), 1.0, 0.0).astype(bf16)
    high, mid, low = split3(pos_ref[...])
    nt = ((1,), (1,))
    tail = (dot(eye3, high, nt) + dot(eye3, mid, nt)) + dot(eye3, low, nt)
    lane, slot = iota((8, 256), 1), iota((8, 256), 0)
    total = jnp.zeros((4, 256), f32)
    for i in range(8):
        pick = jnp.where((lane % 8 == slot) & (lane // 32 == i), 1.0, 0.0).astype(bf16)
        total = total + dot(spec_ref[i].astype(f32).astype(bf16), pick)
    keep = (iota((4, 256), 1) // 8) % 4 == iota((4, 256), 0)
    species = jnp.sum(jnp.where(keep, total, 0.0), 0, keepdims=True)
    own_ref[32:40, :] = jnp.where(iota((8, 256), 0) == 3, species, tail)

    lower = lanes((40, L)) < 64
    first, second = own_ref[:, 0:128], own_ref[:, 128:256]
    rows_low = jnp.where(lower, first, roll(second, 64))
    rows_high = jnp.where(lower, roll(first, 64), second)
    front = gz_ref[0] == 0
    straight_ref[...] = jnp.where(front, rows_high, rows_low)
    cross_ref[...] = jnp.where(front, rows_low, rows_high)


def spread(half0, half1, start):
    quarter = lanes((40, L)) // 32
    out = roll(half0, -start)
    out = jnp.where(quarter == 1, roll(half1, 32 - start), out)
    out = jnp.where(quarter == 2, roll(half0, 32 - start), out)
    return jnp.where(quarter == 3, roll(half1, 64 - start), out)


def halves(first, second):
    return roll(jnp.where(lanes(first.shape) >= 64, first, second), 64)


def rows_kernel(gz_ref, all_ref, straight_ref, cross_ref, left_ref, right_ref):
    front = gz_ref[0] == 0
    near0 = jnp.where(front, straight_ref[...], cross_ref[...])
    near1 = jnp.where(front, cross_ref[...], straight_ref[...])
    for x in range(2):
        near = spread(near0, near1, 64 * x)
        own = [
            spread(all_ref[0, :, x * L : (x + 1) * L], all_ref[1, :, x * L : (x + 1) * L], 64 * pair)
            for pair in range(2)
        ]
        tiles = [
            jnp.where(front, near, own[0]),
            jnp.where(front, own[0], own[1]),
            jnp.where(front, own[1], near),
        ]
        for pair in range(3):
            at = (x * 3 + pair) * 4
            left_ref[at : at + 4, :] = tiles[pair][32:36]
            right_ref[at : at + 4, :] = tiles[pair][32:36]
        out = left_ref if x == 0 else right_ref
        for r in range(2):
            out[24 + 32 * r : 56 + 32 * r, :] = halves(tiles[r][0:32], tiles[r + 1][0:32])


def weights_kernel(emb_ref, rad_ref, mix_ref, read_ref, vf_ref, vb_ref, wf_ref, wb_ref, mf_ref, mb_ref, et_ref, ro_ref):
    emb = emb_ref[...]
    for q in range(3):
        base = rad_ref[0, :, q * C : (q + 1) * C] * SCALE
        v = jnp.concatenate([base * emb[k : k + 1] for k in range(4)], 0)
        high, low = split2(v)
        vb_ref[q, 0:32, 0:128] = high
        vb_ref[q, 0:32, 128:256] = high
        vb_ref[q, 32:64, 0:128] = low
        vb_ref[q, 32:64, 128:256] = jnp.zeros((32, 128), bf16)
        vt = v.T
        high, low = split2(vt)
        vf_ref[q] = jnp.concatenate([high.astype(f32), high.astype(f32), low.astype(f32)], 1).astype(bf16)
        w = rad_ref[1, :, q * C : (q + 1) * C]
        high, low = split2(w)
        both = jnp.concatenate([high.astype(f32), low.astype(f32)], 0)
        wb_ref[q, :, 0:128] = both.astype(bf16)
        wb_ref[q, :, 128:256] = jnp.where(iota((16, 128), 0) < 8, both, 0.0).astype(bf16)
        high, low = split2(w.T)
        wf_ref[q * C : (q + 1) * C, :] = jnp.concatenate(
            [high.astype(f32), high.astype(f32), low.astype(f32)], 1
        ).astype(bf16)
    for layer in range(2):
        for q in range(3):
            m = mix_ref[layer, q * C : (q + 1) * C, :]
            high, low = split2(m)
            mb_ref[layer, q * C : (q + 1) * C, 0:128] = high
            mb_ref[layer, q * C : (q + 1) * C, 128:256] = high
            mb_ref[layer, q * C : (q + 1) * C, 256:384] = low
            high, low = split2(m.T)
            mf_ref[layer, :, q * C : (q + 1) * C] = high
            mf_ref[layer, :, 384 + q * C : 384 + (q + 1) * C] = high
            mf_ref[layer, :, 768 + q * C : 768 + (q + 1) * C] = low
    high, mid, low = split3(emb)
    stack = jnp.concatenate([high.astype(f32), mid.astype(f32), low.astype(f32), jnp.zeros((4, C), f32)], 0)
    et_ref[...] = stack.T.astype(bf16)
    ro_ref[...] = jnp.broadcast_to(read_ref[...], (C, L)).T


def decode(ids):
    cell = ids >> 3
    ox = (cell >= 9).astype(i32) + (cell >= 18).astype(i32)
    rest = cell - 9 * ox
    oy = (rest >= 3).astype(i32) + (rest >= 6).astype(i32)
    oz = rest - 3 * oy
    lane = lanes(ids.shape)
    ys = (lane >> 6) + oy
    zs = ((lane >> 3) + oz + 7) & 7
    tile = ox * 2 + (ys >> 1)
    target = ((ys & 1) << 6) | (zs << 3) | (ids & 7)
    return ox, oy, oz, tile, target


PX, PY, PZ, RAD, RINV, UM, TM, SP, TILE, TARGET, Y1X, Y1Y, Y1Z, Y20, Y21, Y22, Y23, Y24 = range(18)
ORDERS = ((Y1X, Y1Y, Y1Z), (Y20, Y21, Y22, Y23, Y24))


def harmonics(geo, at, px, py, pz):
    geo[at, Y1X] = R3 * px
    geo[at, Y1Y] = R3 * py
    geo[at, Y1Z] = R3 * pz
    geo[at, Y20] = R15 * px * py
    geo[at, Y21] = R15 * py * pz
    geo[at, Y22] = (0.5 * R5) * (2.0 * pz * pz - px * px - py * py)
    geo[at, Y23] = R15 * px * pz
    geo[at, Y24] = (0.5 * R15) * (px * px - py * py)


def silu_parts(v):
    gate = 1.0 / (1.0 + jnp.exp(-v))
    return v * gate, gate * (1.0 + v * (1.0 - gate))


def main_kernel(
    off_ref, lown_ref, rown_ref, froml_ref, fromr_ref,
    vf_ref, vb_ref, wf_ref, wb_ref, mf_ref, mb_ref, et_ref, ro_ref,
    outl_ref, outo_ref, outr_ref,
    table, edges, geo, basis, slope, moment, hid, dsilu, dhid, dmom, inv, geo2, rb2, rbst, hg, onehot,
    hs, rad2, efac, dhs, drad, extra, pick, force,
):
    for plane, (ref, base) in enumerate(
        ((froml_ref, 0), (froml_ref, 1), (lown_ref, 0), (lown_ref, 1), (fromr_ref, 0), (fromr_ref, 1))
    ):
        for pair in range(3):
            at = (base * 3 + pair) * 4
            table[plane * 3 + pair, 0:4, :] = ref[at : at + 4, :]
    for plane, ref in enumerate((froml_ref, lown_ref, rown_ref, fromr_ref)):
        for r in range(2):
            edges[plane * 2 + r] = ref[24 + 32 * r : 56 + 32 * r, :]

    centre = iota((NB, L), 0).astype(f32) * (CUT / (NB - 1))
    lane8 = lanes((8, L))

    def layer_one(xr, _):
        kinds = []
        for r in range(2):
            at = xr * 2 + r
            own_a = table[(xr + 1) * 3 + r]
            own_b = table[(xr + 1) * 3 + r + 1]
            own = halves(own_a, own_b)
            kinds.append(own[3:4])
            ids = edges[at, 0:16, :].astype(i32)
            ox, oy, oz, tile, target = decode(ids)
            got = [jnp.zeros((E, L), f32) for _ in range(4)]
            for t in range(6):
                src = table[(xr + t // 2) * 3 + r + t % 2]
                here = tile == t
                for q in range(4):
                    wide = jnp.broadcast_to(src[q : q + 1], (E, L))
                    val = jnp.take_along_axis(wide, target, axis=1, mode="promise_in_bounds")
                    got[q] = jnp.where(here, val, got[q])
            dx = ((ox - 1).astype(f32) + got[0]) - own[0:1]
            dy = ((oy - 1).astype(f32) + got[1]) - own[1:2]
            dz = ((oz - 1).astype(f32) + got[2]) - own[2:3]
            sq = dx * dx + dy * dy + dz * dz
            rinv = lax.rsqrt(sq)
            dist = jnp.sqrt(sq)
            mask = edges[at, 16:32, :]
            part = jnp.where(dist < CUT, 1.0 - sq * (1.0 / CUT**2), 0.0) * mask
            px, py, pz = 0.5 * dx, 0.5 * dy, 0.5 * dz
            geo[at, PX] = px
            geo[at, PY] = py
            geo[at, PZ] = pz
            geo[at, RAD] = dist
            geo[at, RINV] = rinv
            geo[at, UM] = part * part
            geo[at, TM] = part
            geo[at, SP] = got[3]
            geo[at, TILE] = tile.astype(f32)
            geo[at, TARGET] = target.astype(f32)
            harmonics(geo, at, px, py, pz)

            acc = [[None] * 4 for _ in range(9)]
            for e in range(E):
                def row(i):
                    return jnp.broadcast_to(geo[at, i, e : e + 1, :], (NB, L))

                diff = row(RAD) - centre
                bump = jnp.exp(-GAMMA * (diff * diff))
                rb = bump * row(UM)
                basis[at, e * 8 : e * 8 + 8, :] = rb
                slope[at, e * 8 : e * 8 + 8, :] = -(bump * row(TM)) - (2.0 * GAMMA) * (diff * rb * row(RINV))
                kind = row(SP)
                per = [jnp.where(kind == float(k), rb, 0.0) for k in range(4)]
                for qm in range(9):
                    y = None if qm == 0 else row(Y1X + qm - 1)
                    for k in range(4):
                        term = per[k] if y is None else y * per[k]
                        acc[qm][k] = term if e == 0 else acc[qm][k] + term
            first = 0
            for q, count in enumerate((1, 3, 5)):
                blocks = []
                for m in range(count):
                    p = jnp.concatenate(acc[first + m], 0)
                    high, low = split2(p)
                    blocks.append(jnp.concatenate([high, low, high], 0))
                first += count
                out = dot(vf_ref[q], jnp.concatenate(blocks, 1) if count > 1 else blocks[0])
                if q == 0:
                    value = out
                else:
                    value = None
                    for m in range(count):
                        a = out[:, m * L : (m + 1) * L]
                        moment[at, (0, 3)[q - 1] + m] = a
                        value = a * a if value is None else value + a * a
                high, low = split2(value)
                inv[q * C : (q + 1) * C, r * L : (r + 1) * L] = high
                inv[384 + q * C : 384 + (q + 1) * C, r * L : (r + 1) * L] = low
                inv[768 + q * C : 768 + (q + 1) * C, r * L : (r + 1) * L] = high
        z = dot(mf_ref[0], inv[...])
        update, slope_z = silu_parts(z)
        kind = jnp.concatenate([jnp.broadcast_to(k, (16, L)) for k in kinds], 1)
        sel = iota((16, 2 * L), 0)
        hot = jnp.where((kind == (sel % 4).astype(f32)) & (sel < 12), 1.0, 0.0).astype(bf16)
        h1 = dot(et_ref[...], hot) + update
        for r in range(2):
            hid[xr * 2 + r] = h1[:, r * L : (r + 1) * L]
            dsilu[xr * 2 + r] = slope_z[:, r * L : (r + 1) * L]
        return 0

    lax.fori_loop(0, 4, layer_one, 0)

    read = ro_ref[...]
    low_half = lanes((C, L)) < 64
    for plane in range(4):
        for r in range(2):
            if plane in (1, 2):
                keep = low_half if r == 1 else ~low_half
                dhid[plane * 2 + r] = jnp.where(keep, read, 0.0)
            else:
                dhid[plane * 2 + r] = jnp.zeros((C, L), f32)

    def layer_two(x, _):
        a, b = (x + 1) * 2, (x + 1) * 2 + 1
        ids = halves(edges[a, 0:16, :], edges[b, 0:16, :]).astype(i32)
        _, _, _, tile, target = decode(ids)
        geo2[TILE] = tile.astype(f32)
        geo2[TARGET] = target.astype(f32)
        for i in (PX, PY, PZ, Y1X, Y1Y, Y1Z, Y20, Y21, Y22, Y23, Y24):
            geo2[i] = halves(geo[a, i], geo[b, i])
        rb2[...] = halves(basis[a], basis[b])
        for e in range(E):
            high, low = split2(rb2[e * 8 : e * 8 + 8, :])
            high = high.astype(f32)
            rbst[:, e * L : (e + 1) * L] = jnp.concatenate([high, low.astype(f32), high], 0).astype(bf16)
        for t in range(6):
            h = hid[(x + t // 2) * 2 + t % 2]
            high, low = split2(h)
            hg[0:128, t * L : (t + 1) * L] = high
            hg[128:256, t * L : (t + 1) * L] = low
        spot = iota((C, L), 0).astype(f32).astype(bf16)
        one, zero = jnp.ones((), bf16), jnp.zeros((), bf16)
        for e in range(E):
            where_t = geo2[TILE, e : e + 1, :]
            where_l = geo2[TARGET, e : e + 1, :]
            for t in range(6):
                code = jnp.where(where_t == float(t), where_l, -1.0).astype(bf16)
                hot = jnp.where(spot == jnp.broadcast_to(code, (C, L)), one, zero)
                onehot[t * L : (t + 1) * L, e * L : (e + 1) * L] = hot

        def gather(i, _):
            at = pl.ds(pl.multiple_of(i * 256, 256), 256)
            out = dot(hg[...], onehot[:, at])
            hs[:, at] = out[0:128] + out[128:256]
            rad2[:, at] = dot(wf_ref[...], rbst[:, at])
            return 0

        lax.fori_loop(0, 8, gather, 0)

        def contract(i, _):
            rows = pl.multiple_of(i * 16, 16)
            acc = [None] * 9
            for e in range(E):
                cols = slice(e * L, (e + 1) * L)
                h = hs[pl.ds(rows, 16), cols]
                ts = [rad2[pl.ds(q * C + rows, 16), cols] * h for q in range(3)]
                for qm in range(9):
                    if qm == 0:
                        term = ts[0]
                    else:
                        y = jnp.broadcast_to(geo2[Y1X + qm - 1, e : e + 1, :], (16, L))
                        term = y * ts[1 if qm < 4 else 2]
                    acc[qm] = term if e == 0 else acc[qm] + term
            for qm in range(9):
                efac[qm, pl.ds(rows, 16), :] = acc[qm] * SCALE
            return 0

        lax.fori_loop(0, 8, contract, 0)

        one_sq = efac[1] * efac[1] + efac[2] * efac[2] + efac[3] * efac[3]
        two_sq = efac[4] * efac[4]
        for m in range(5, 9):
            two_sq = two_sq + efac[m] * efac[m]
        for q, value in enumerate((efac[0], one_sq, two_sq)):
            high, low = split2(value)
            inv[q * C : (q + 1) * C, 0:128] = high
            inv[384 + q * C : 384 + (q + 1) * C, 0:128] = low
            inv[768 + q * C : 768 + (q + 1) * C, 0:128] = high
        z = dot(mf_ref[1], inv[:, 0:128])
        update, slope_z = silu_parts(z)
        h2 = halves(hid[a], hid[b]) + update
        kind = table[(x + 2) * 3 + 1, 3:4, :]
        offset = jnp.zeros((1, L), f32)
        for k in range(4):
            offset = jnp.where(kind == float(k), off_ref[k], offset)
        energy = jnp.sum(read * h2, 0, keepdims=True) + offset
        geo2[RAD, 0:1, :] = energy
        extra[x, 0, 0, 0:1, :] = energy

        high, low = split2(read * slope_z)
        dinv = dot(mb_ref[1], jnp.concatenate([high, low, high], 0))
        efac[0] = dinv[0:128] * SCALE
        for m in range(1, 9):
            part = dinv[128:256] if m < 4 else dinv[256:384]
            efac[m] = efac[m] * part * (2.0 * SCALE)

        def back(e, _):
            cols = pl.ds(pl.multiple_of(e * L, L), L)

            def row(i):
                return jnp.broadcast_to(geo2[i, pl.ds(e, 1), :], (16, L))

            ys = [None] + [row(Y1X + m) for m in range(8)]
            acc = [None] * 9
            for i in range(8):
                rows = slice(i * 16, i * 16 + 16)
                h = hs[rows, cols]
                rr = [rad2[q * C + i * 16 : q * C + i * 16 + 16, cols] for q in range(3)]
                ef = [efac[qm, rows, :] for qm in range(9)]
                d0 = ef[0]
                d1 = ys[1] * ef[1] + ys[2] * ef[2] + ys[3] * ef[3]
                d2 = ys[4] * ef[4] + ys[5] * ef[5] + ys[6] * ef[6] + ys[7] * ef[7] + ys[8] * ef[8]
                t1 = rr[1] * h
                t2 = rr[2] * h
                for qm in range(1, 9):
                    term = (t1 if qm < 4 else t2) * ef[qm]
                    acc[qm] = term if i == 0 else acc[qm] + term
                high, low = split2(d0 * rr[0] + d1 * rr[1] + d2 * rr[2])
                dhs[rows, cols] = high
                dhs[128 + i * 16 : 144 + i * 16, cols] = low
                for q, d in enumerate((d0, d1, d2)):
                    high, low = split2(d * h)
                    drad[q, rows, cols] = high
                    drad[q, 128 + i * 16 : 144 + i * 16, cols] = low
            fold = [None] + [acc[m][0:8] + acc[m][8:16] for m in range(1, 9)]
            px, py, pz = (jnp.broadcast_to(geo2[i, pl.ds(e, 1), :], (8, L)) for i in (PX, PY, PZ))
            gx = R3 * fold[1] + R15 * (py * fold[4] + pz * fold[7] + px * fold[8]) - R5 * (px * fold[6])
            gy = R3 * fold[2] + R15 * (px * fold[4] + pz * fold[5] - py * fold[8]) - R5 * (py * fold[6])
            gz = R3 * fold[3] + R15 * (py * fold[5] + px * fold[7]) + (2.0 * R5) * (pz * fold[6])
            extra[x, e + 1, 1] = roll(0.5 * gx, 64)
            extra[x, e + 1, 2] = roll(0.5 * gy, 64)
            extra[x, e + 1, 3] = roll(0.5 * gz, 64)
            return 0

        lax.fori_loop(0, E, back, 0)

        grad = dot(wb_ref[0], drad[0]) + dot(wb_ref[1], drad[1]) + dot(wb_ref[2], drad[2])
        for e in range(E):
            g = grad[0:8, e * L : (e + 1) * L] + grad[8:16, e * L : (e + 1) * L]
            extra[x, e + 1, 0] = roll(g, 64)
        for t in range(6):
            out = dot(dhs[...], onehot[t * L : (t + 1) * L, :], ((1,), (1,)))
            at = (x + t // 2) * 2 + t % 2
            dhid[at] = dhid[at] + (out[0:128] + out[128:256])
        return 0

    lax.fori_loop(0, 2, layer_two, 0)

    for i in range(18):
        force[i] = jnp.zeros((8, L), f32)
    sub8 = iota((8, L), 0)
    spot = iota((C, L), 0).astype(f32).astype(bf16)
    one, zero = jnp.ones((), bf16), jnp.zeros((), bf16)

    def layer_one_back(xr, _):
        inner = (xr == 1) | (xr == 2)
        x_own = jnp.clip(xr - 1, 0, 1)
        dz = jnp.concatenate([dhid[xr * 2 + r] * dsilu[xr * 2 + r] for r in range(2)], 1)
        high, low = split2(dz)
        dinv = dot(mb_ref[0], jnp.concatenate([high, low, high], 0))
        for r in range(2):
            at = xr * 2 + r
            cols = slice(r * L, (r + 1) * L)
            first = 0
            for q, count in enumerate((1, 3, 5)):
                part = dinv[q * C : (q + 1) * C, cols]
                blocks = []
                for m in range(count):
                    da = part if q == 0 else 2.0 * moment[at, (0, 3)[q - 1] + m] * part
                    high, low = split2(da)
                    blocks.append(jnp.concatenate([high, low], 0))
                out = dot(vb_ref[q], jnp.concatenate(blocks, 1) if count > 1 else blocks[0])
                for m in range(count):
                    one_m = out[:, m * L : (m + 1) * L]
                    dmom[first + m] = one_m[0:32] + one_m[32:64]
                first += count
            keep = ((lane8 >= 64) if r == 0 else (lane8 < 64)) & inner
            received = jnp.zeros((8, L), f32)
            for e in range(E):
                def row(i):
                    return jnp.broadcast_to(geo[at, i, e : e + 1, :], (NB, L))

                kind = row(SP)
                is0, is1, is2 = kind == 0.0, kind == 1.0, kind == 2.0
                dp = []
                for qm in range(9):
                    sel = jnp.where(is2, dmom[qm, 16:24, :], dmom[qm, 24:32, :])
                    sel = jnp.where(is1, dmom[qm, 8:16, :], sel)
                    dp.append(jnp.where(is0, dmom[qm, 0:8, :], sel))
                rb = basis[at, e * 8 : e * 8 + 8, :]
                g = dp[0]
                for m in range(8):
                    g = g + row(Y1X + m) * dp[m + 1]
                g = g + jnp.where(keep, extra[x_own, e + 1, 0], 0.0)
                radial = (2.0 * g) * slope[at, e * 8 : e * 8 + 8, :]
                px, py, pz = row(PX), row(PY), row(PZ)
                c22 = dp[6] * (1.0 / R3)
                half = (0.5 * R15) * rb
                hr = (0.5 * R3) * rb
                gx = px * radial + hr * dp[1] + half * (py * dp[4] + pz * dp[7] + px * (dp[8] - c22))
                gy = py * radial + hr * dp[2] + half * (px * dp[4] + pz * dp[5] - py * (dp[8] + c22))
                gz = pz * radial + hr * dp[3] + half * (py * dp[5] + px * dp[7] + pz * (c22 + c22))
                gx = gx + jnp.where(keep, extra[x_own, e + 1, 1], 0.0)
                gy = gy + jnp.where(keep, extra[x_own, e + 1, 2], 0.0)
                gz = gz + jnp.where(keep, extra[x_own, e + 1, 3], 0.0)
                sx = jnp.sum(gx, 0, keepdims=True)
                sy = jnp.sum(gy, 0, keepdims=True)
                sz = jnp.sum(gz, 0, keepdims=True)
                vec = jnp.where(sub8 == 0, sx, jnp.where(sub8 == 1, sy, jnp.where(sub8 == 2, sz, 0.0)))
                received = received + vec
                high, low = split2(vec)
                both = jnp.concatenate([high.astype(f32), low.astype(f32)], 0)
                where_t = jnp.broadcast_to(geo[at, TILE, e : e + 1, :], (16, L))
                for t in range(6):
                    pick[t * 16 : (t + 1) * 16, e * L : (e + 1) * L] = jnp.where(
                        where_t == float(t), both, 0.0
                    ).astype(bf16)
                code = jnp.broadcast_to(geo[at, TARGET, e : e + 1, :].astype(bf16), (C, L))
                onehot[0:128, e * L : (e + 1) * L] = jnp.where(spot == code, one, zero)
            sent = dot(pick[...], onehot[0:128, :], ((1,), (1,)))
            for t in range(6):
                to = (xr + t // 2) * 3 + r + t % 2
                force[to] = force[to] - (sent[t * 16 : t * 16 + 8] + sent[t * 16 + 8 : t * 16 + 16])
            turned = roll(received, 64)
            mine = (xr + 1) * 3 + r
            force[mine] = force[mine] + jnp.where(lane8 >= 64, turned, 0.0)
            force[mine + 1] = force[mine + 1] + jnp.where(lane8 < 64, turned, 0.0)
        return 0

    lax.fori_loop(0, 4, layer_one_back, 0)

    for plane in range(6):
        for pair in range(3):
            out = (outl_ref, outo_ref, outr_ref)[plane // 2]
            at = ((plane % 2) * 3 + pair) * 4
            out[at : at + 4, :] = force[plane * 3 + pair, 0:4, :]
            if plane in (2, 3) and pair == 1:
                out[at + 3 : at + 4, :] = extra[plane - 2, 0, 0, 0:1, :]


def chunk_kernel(place_ref, own_ref, left_ref, right_ref, out_ref):
    gy, gz = place_ref[0], place_ref[1]
    front = gz == 0
    total = own_ref[...] + left_ref[...] + right_ref[...]
    quarter = lanes((4, L)) // 32

    def squeeze(pair, zh):
        first = total[pair * 4 : pair * 4 + 4]
        second = total[12 + pair * 4 : 16 + pair * 4]
        out = roll(first, -32 * zh)
        out = jnp.where(quarter == 1, roll(first, -32 - 32 * zh), out)
        out = jnp.where(quarter == 2, roll(second, 64 - 32 * zh), out)
        return jnp.where(quarter == 3, roll(second, 32 - 32 * zh), out)

    out_ref[...] = jnp.zeros(out_ref.shape, f32)
    y_count = out_ref.shape[0] // 2
    beside = jnp.where(front, gy + y_count - 1, gy + 1)
    beside = jnp.where(beside >= y_count, beside - y_count, beside)
    for zh in range(2):
        parts = [squeeze(pair, zh) for pair in range(3)]
        low = jnp.where(front, parts[1], parts[0])
        high = jnp.where(front, parts[2], parts[1])
        near = jnp.where(front, parts[0], parts[2])
        out_ref[gy * 2 + zh] = jnp.concatenate([low, high], 0)
        out_ref[beside * 2 + zh, 0:4, :] = near


def unpack_kernel(place_ref, got_ref, energy_ref, force_ref):
    gy = place_ref[0]
    y_count = got_ref.shape[0] // 2
    below = jnp.where(gy == 0, y_count - 1, gy - 1)
    above = jnp.where(gy == y_count - 1, 0, gy + 1)
    own = got_ref[gy * 2] + got_ref[gy * 2 + 1]
    low = own[0:4] + got_ref[below * 2 + 1, 0:4, :]
    high = own[4:8] + got_ref[above * 2, 0:4, :]
    lower = lanes((4, L)) < 64
    first = jnp.where(lower, low, roll(high, 64))
    second = jnp.where(lower, roll(low, 64), high)
    rows = jnp.concatenate([first, second], 1)
    rows8 = jnp.concatenate([rows, jnp.zeros((4, 256), f32)], 0)
    force_ref[...] = rows8.T[:, 0:3]
    pick = jnp.where(iota((8, 256), 1) % 8 == iota((8, 256), 0), 1.0, 0.0).astype(bf16)
    high, mid, low = split3(rows[3:4])
    lane, cell = iota((4, 256), 1), iota((4, 256), 0)
    nt = ((1,), (1,))
    for i in range(8):
        keep = lane // 8 == cell + 4 * i
        total = None
        for part in (high, mid, low):
            piece = dot(jnp.where(keep, part.astype(f32), 0.0).astype(bf16), pick, nt)
            total = piece if total is None else total + piece
        energy_ref[i] = total


def call(kernel, outs, in_specs, scratch=(), flops=10**6):
    return pl.pallas_call(
        kernel,
        out_shape=outs,
        in_specs=in_specs,
        out_specs=jax.tree.map(lambda _: pl.BlockSpec(memory_space=VMEM), outs),
        scratch_shapes=list(scratch),
        compiler_params=pltpu.CompilerParams(vmem_limit_bytes=60 * 2**20),
        cost_estimate=pl.CostEstimate(flops=flops, bytes_accessed=10**5, transcendentals=0),
    )


def shape(*dims, dtype=f32):
    return jax.ShapeDtypeStruct(dims, dtype)


def shards(
    positions, species, neighbors, edge_mask, species_embed, radial_weight, mix_weight, readout, energy_offset
):
    v = pl.BlockSpec(memory_space=VMEM)
    sm = pl.BlockSpec(memory_space=SMEM)
    gy_count, gz_count = lax.axis_size("gy"), lax.axis_size("gz")
    gx_count = lax.axis_size("gx")
    gy, gz = lax.axis_index("gy"), lax.axis_index("gz")
    place = jnp.stack([gy, gz]).astype(i32)
    gz_only = gz.astype(i32).reshape(1)

    own, straight, cross = call(
        pack_kernel, [shape(40, 256), shape(40, L), shape(40, L)], [sm, v, v, v, v]
    )(
        gz_only,
        positions.reshape(256, 3),
        species.reshape(8, 4, 8),
        neighbors.reshape(256, E),
        edge_mask.reshape(256, E),
    )

    def dev(y, s):
        return (y % gy_count) * gz_count + s

    yz = ("gy", "gz")
    go_straight = [(dev(y, s), dev(y + 1 if s == 0 else y - 1, s)) for y in range(gy_count) for s in range(2)]
    go_cross = [(dev(y, s), dev(y - 1 if s == 0 else y + 1, 1 - s)) for y in range(gy_count) for s in range(2)]
    near_straight = lax.ppermute(straight, yz, go_straight)
    near_cross = lax.ppermute(cross, yz, go_cross)
    both = lax.all_gather(own, "gz")

    left, right = call(rows_kernel, [shape(88, L), shape(88, L)], [sm, v, v, v])(
        gz_only, both, near_straight, near_cross
    )
    up = [(i, (i + 1) % gx_count) for i in range(gx_count)]
    down = [(j, i) for i, j in up]
    from_left = lax.ppermute(right, "gx", up)
    from_right = lax.ppermute(left, "gx", down)

    weights = call(
        weights_kernel,
        [
            shape(3, C, 96, dtype=bf16),
            shape(3, 64, 256, dtype=bf16),
            shape(384, 24, dtype=bf16),
            shape(3, 16, 256, dtype=bf16),
            shape(2, C, 1152, dtype=bf16),
            shape(2, 384, 384, dtype=bf16),
            shape(C, 16, dtype=bf16),
            shape(C, L),
        ],
        [v, v, v, v],
        flops=10**7,
    )(species_embed, radial_weight, mix_weight, readout.reshape(1, C))

    scratch = [
        VMEM((18, 8, L), f32),
        VMEM((8, 32, L), f32),
        VMEM((8, 18, E, L), f32),
        VMEM((8, 128, L), f32),
        VMEM((8, 128, L), f32),
        VMEM((8, 8, C, L), f32),
        VMEM((8, C, L), f32),
        VMEM((8, C, L), f32),
        VMEM((8, C, L), f32),
        VMEM((9, 32, L), f32),
        VMEM((1152, 256), bf16),
        VMEM((18, E, L), f32),
        VMEM((128, L), f32),
        VMEM((24, E * L), bf16),
        VMEM((256, 768), bf16),
        VMEM((768, E * L), bf16),
        VMEM((C, E * L), f32),
        VMEM((384, E * L), f32),
        VMEM((9, C, L), f32),
        VMEM((256, E * L), bf16),
        VMEM((3, 256, E * L), bf16),
        VMEM((2, E + 1, 4, 8, L), f32),
        VMEM((96, E * L), bf16),
        VMEM((18, 8, L), f32),
    ]
    out_left, out_own, out_right = call(
        main_kernel, [shape(24, L)] * 3, [sm] + [v] * 12, scratch, flops=10**9
    )(energy_offset, left, right, from_left, from_right, *weights)

    back_right = lax.ppermute(out_left, "gx", down)
    back_left = lax.ppermute(out_right, "gx", up)
    chunks = call(chunk_kernel, shape(gy_count * 2, 8, L), [sm, v, v, v])(place, out_own, back_left, back_right)
    got = lax.all_to_all(chunks, yz, 0, 0)
    energy, force = call(unpack_kernel, [shape(8, 4, 8), shape(256, 3)], [sm, v])(place, got)
    return energy.reshape(2, 4, 4, 8), force.reshape(2, 4, 4, 8, 3)


def solution(mesh):
    in_specs = (
        P("gx", "gy", "gz", None, None),
        P("gx", "gy", "gz", None),
        P("gx", "gy", "gz", None, None),
        P("gx", "gy", "gz", None, None),
        P(),
        P(),
        P(),
        P(),
        P(),
    )
    out_specs = (P("gx", "gy", "gz", None), P("gx", "gy", "gz", None, None))
    return jax.shard_map(shards, mesh=mesh, in_specs=in_specs, out_specs=out_specs, check_vma=False)
```

```python
import math

import jax
import jax.numpy as jnp
from jax import lax
from jax.experimental import pallas as pl
from jax.experimental.pallas import tpu as pltpu
from jax.sharding import PartitionSpec as P

f32 = jnp.float32
bf16 = jnp.bfloat16
i32 = jnp.int32

E = 16
C = 128
NB = 8
L = 128
CUT = 2.0
GAMMA = ((NB - 1) / CUT) ** 2
SCALE = E**-0.5
R3 = math.sqrt(3.0)
R5 = math.sqrt(5.0)
R15 = math.sqrt(15.0)
VMEM = pltpu.VMEM
SMEM = pltpu.SMEM


def split2(x):
    high = x.astype(bf16)
    low = (x - high.astype(f32)).astype(bf16)
    return high, low


def split3(x):
    high = x.astype(bf16)
    rest = x - high.astype(f32)
    mid = rest.astype(bf16)
    low = (rest - mid.astype(f32)).astype(bf16)
    return high, mid, low


def dot(a, b, dims=((1,), (0,))):
    return lax.dot_general(a, b, (dims, ((), ())), preferred_element_type=f32)


def iota(shape, dim):
    return lax.broadcasted_iota(i32, shape, dim)


def roll(x, shift):
    return pltpu.roll(x, shift % x.shape[-1], x.ndim - 1)


def lanes(shape):
    return iota(shape, len(shape) - 1)


def block_masks(count):
    row, lane = iota((32 * count, 256), 0), iota((32 * count, 256), 1)
    keep = (lane // 32 == row // (4 * count)) & ((lane // 8) % 4 == row % 4)
    spread8 = jnp.where(iota((8, 256), 1) % 8 == iota((8, 256), 0), 1.0, 0.0).astype(bf16)
    return keep, spread8


def pack_kernel(
    gz_ref, pos_hbm, spec_hbm, nbr_hbm, mask_hbm, own_ref, straight_ref, cross_ref, pos_ref, spec_ref, nbr_ref, mask_ref, sems
):
    copies = [
        pltpu.make_async_copy(src, dst, sems.at[i])
        for i, (src, dst) in enumerate(
            ((nbr_hbm, nbr_ref), (mask_hbm, mask_ref), (pos_hbm, pos_ref), (spec_hbm, spec_ref))
        )
    ]
    for copy in copies:
        copy.start()
    for copy in copies:
        copy.wait()
    eye16 = jnp.where(iota((E, E), 0) == iota((E, E), 1), 1.0, 0.0).astype(bf16)
    own_ref[0:16, :] = dot(eye16, nbr_ref[...].astype(f32).astype(bf16), ((1,), (1,)))
    own_ref[16:32, :] = dot(eye16, mask_ref[...].astype(f32).astype(bf16), ((1,), (1,)))
    keep, spread8 = block_masks(3)
    group = jnp.where((iota((8, 96), 1) // 4) % 3 == iota((8, 96), 0), 1.0, 0.0).astype(bf16)
    tail = None
    for part in split3(pos_ref[...]):
        rows = jnp.where(keep, dot(part, spread8), 0.0).astype(bf16)
        piece = dot(group, rows)
        tail = piece if tail is None else tail + piece
    keep, _ = block_masks(1)
    kinds = jnp.where(keep, dot(spec_ref[...].astype(f32).astype(bf16), spread8), 0.0)
    species = jnp.sum(kinds, 0, keepdims=True)
    own_ref[32:40, :] = jnp.where(iota((8, 256), 0) == 3, species, tail)

    lower = lanes((40, L)) < 64
    first, second = own_ref[:, 0:128], own_ref[:, 128:256]
    rows_low = jnp.where(lower, first, roll(second, 64))
    rows_high = jnp.where(lower, roll(first, 64), second)
    front = gz_ref[0] == 0
    straight_ref[...] = jnp.where(front, rows_high, rows_low)
    cross_ref[...] = jnp.where(front, rows_low, rows_high)


def spread(half0, half1, start):
    quarter = lanes((40, L)) // 32
    out = roll(half0, -start)
    out = jnp.where(quarter == 1, roll(half1, 32 - start), out)
    out = jnp.where(quarter == 2, roll(half0, 32 - start), out)
    return jnp.where(quarter == 3, roll(half1, 64 - start), out)


def halves(first, second):
    return roll(jnp.where(lanes(first.shape) >= 64, first, second), 64)


def rows_kernel(gz_ref, all_ref, straight_ref, cross_ref, left_ref, right_ref):
    front = gz_ref[0] == 0
    near0 = jnp.where(front, straight_ref[...], cross_ref[...])
    near1 = jnp.where(front, cross_ref[...], straight_ref[...])
    for x in range(2):
        near = spread(near0, near1, 64 * x)
        own = [
            spread(all_ref[0, :, x * L : (x + 1) * L], all_ref[1, :, x * L : (x + 1) * L], 64 * pair)
            for pair in range(2)
        ]
        tiles = [
            jnp.where(front, near, own[0]),
            jnp.where(front, own[0], own[1]),
            jnp.where(front, own[1], near),
        ]
        for pair in range(3):
            at = (x * 3 + pair) * 4
            left_ref[at : at + 4, :] = tiles[pair][32:36]
            right_ref[at : at + 4, :] = tiles[pair][32:36]
        out = left_ref if x == 0 else right_ref
        for r in range(2):
            out[24 + 32 * r : 56 + 32 * r, :] = halves(tiles[r][0:32], tiles[r + 1][0:32])


def weights_kernel(
    emb_ref, rad_ref, mix_ref, read_ref, off_ref, vf_ref, vb_ref, wf_ref, wb_ref, mf_ref, mb_ref, et_ref, ro_ref, eo_ref
):
    emb = emb_ref[...]
    for q in range(3):
        base = rad_ref[0, :, q * C : (q + 1) * C] * SCALE
        v = jnp.concatenate([base * emb[k : k + 1] for k in range(4)], 0)
        high, low = split2(v)
        vb_ref[q, 0:32, 0:128] = high
        vb_ref[q, 0:32, 128:256] = high
        vb_ref[q, 32:64, 0:128] = low
        vb_ref[q, 32:64, 128:256] = jnp.zeros((32, 128), bf16)
        vt = v.T
        high, low = split2(vt)
        vf_ref[q] = jnp.concatenate([high.astype(f32), high.astype(f32), low.astype(f32)], 1).astype(bf16)
        w = rad_ref[1, :, q * C : (q + 1) * C]
        high, low = split2(w)
        both = jnp.concatenate([high.astype(f32), low.astype(f32)], 0)
        wb_ref[q, :, 0:128] = both.astype(bf16)
        wb_ref[q, :, 128:256] = jnp.where(iota((16, 128), 0) < 8, both, 0.0).astype(bf16)
        high, low = split2(w.T)
        wf_ref[q * C : (q + 1) * C, :] = jnp.concatenate(
            [high.astype(f32), high.astype(f32), low.astype(f32)], 1
        ).astype(bf16)
    for layer in range(2):
        for q in range(3):
            m = mix_ref[layer, q * C : (q + 1) * C, :]
            high, low = split2(m)
            mb_ref[layer, q * C : (q + 1) * C, 0:128] = high
            mb_ref[layer, q * C : (q + 1) * C, 128:256] = high
            mb_ref[layer, q * C : (q + 1) * C, 256:384] = low
            high, low = split2(m.T)
            mf_ref[layer, :, q * C : (q + 1) * C] = high
            mf_ref[layer, :, 384 + q * C : 384 + (q + 1) * C] = high
            mf_ref[layer, :, 768 + q * C : 768 + (q + 1) * C] = low
    high, mid, low = split3(emb)
    stack = jnp.concatenate([high.astype(f32), mid.astype(f32), low.astype(f32), jnp.zeros((4, C), f32)], 0)
    et_ref[...] = stack.T.astype(bf16)
    ro_ref[...] = jnp.broadcast_to(read_ref[...], (C, L)).T
    pick = jnp.where(iota((4, 4), 0) == iota((4, 4), 1), off_ref[...], 0.0)
    eo_ref[...] = jnp.broadcast_to(jnp.sum(pick, 1, keepdims=True), (4, L))


def decode(ids):
    cell = ids >> 3
    ox = (cell >= 9).astype(i32) + (cell >= 18).astype(i32)
    rest = cell - 9 * ox
    oy = (rest >= 3).astype(i32) + (rest >= 6).astype(i32)
    oz = rest - 3 * oy
    lane = lanes(ids.shape)
    ys = (lane >> 6) + oy
    zs = ((lane >> 3) + oz + 7) & 7
    tile = ox * 2 + (ys >> 1)
    target = ((ys & 1) << 6) | (zs << 3) | (ids & 7)
    return ox, oy, oz, tile, target


PX, PY, PZ, RAD, RINV, UM, TM, SP, TILE, TARGET, Y1X, Y1Y, Y1Z, Y20, Y21, Y22, Y23, Y24 = range(18)
ORDERS = ((Y1X, Y1Y, Y1Z), (Y20, Y21, Y22, Y23, Y24))


def harmonics(geo, at, px, py, pz):
    geo[at, Y1X] = R3 * px
    geo[at, Y1Y] = R3 * py
    geo[at, Y1Z] = R3 * pz
    geo[at, Y20] = R15 * px * py
    geo[at, Y21] = R15 * py * pz
    geo[at, Y22] = (0.5 * R5) * (2.0 * pz * pz - px * px - py * py)
    geo[at, Y23] = R15 * px * pz
    geo[at, Y24] = (0.5 * R15) * (px * px - py * py)


def silu_parts(v):
    gate = 1.0 / (1.0 + jnp.exp(-v))
    return v * gate, gate * (1.0 + v * (1.0 - gate))


def main_kernel(
    lown_ref, rown_ref, froml_ref, fromr_ref,
    vf_ref, vb_ref, wf_ref, wb_ref, mf_ref, mb_ref, et_ref, ro_ref, eo_ref,
    outl_ref, outo_ref, outr_ref,
    table, edges, geo, basis, slope, moment, hid, dsilu, dhid, dmom, inv, geo2, rb2, rbst, hg, onehot,
    hs, rad2, efac, dhs, drad, extra, pick, force,
):
    for plane, (ref, base) in enumerate(
        ((froml_ref, 0), (froml_ref, 1), (lown_ref, 0), (lown_ref, 1), (fromr_ref, 0), (fromr_ref, 1))
    ):
        for pair in range(3):
            at = (base * 3 + pair) * 4
            table[plane * 3 + pair, 0:4, :] = ref[at : at + 4, :]
    for plane, ref in enumerate((froml_ref, lown_ref, rown_ref, fromr_ref)):
        for r in range(2):
            edges[plane * 2 + r] = ref[24 + 32 * r : 56 + 32 * r, :]

    centre = iota((NB, L), 0).astype(f32) * (CUT / (NB - 1))
    lane8 = lanes((8, L))

    def layer_one(xr, _):
        kinds = []
        for r in range(2):
            at = xr * 2 + r
            own_a = table[(xr + 1) * 3 + r]
            own_b = table[(xr + 1) * 3 + r + 1]
            own = halves(own_a, own_b)
            kinds.append(own[3:4])
            ids = edges[at, 0:16, :].astype(i32)
            ox, oy, oz, tile, target = decode(ids)
            got = [jnp.zeros((E, L), f32) for _ in range(4)]
            for t in range(6):
                src = table[(xr + t // 2) * 3 + r + t % 2]
                here = tile == t
                for q in range(4):
                    wide = jnp.broadcast_to(src[q : q + 1], (E, L))
                    val = jnp.take_along_axis(wide, target, axis=1, mode="promise_in_bounds")
                    got[q] = jnp.where(here, val, got[q])
            dx = ((ox - 1).astype(f32) + got[0]) - own[0:1]
            dy = ((oy - 1).astype(f32) + got[1]) - own[1:2]
            dz = ((oz - 1).astype(f32) + got[2]) - own[2:3]
            sq = dx * dx + dy * dy + dz * dz
            rinv = lax.rsqrt(sq)
            dist = jnp.sqrt(sq)
            mask = edges[at, 16:32, :]
            part = jnp.where(dist < CUT, 1.0 - sq * (1.0 / CUT**2), 0.0) * mask
            px, py, pz = 0.5 * dx, 0.5 * dy, 0.5 * dz
            geo[at, PX] = px
            geo[at, PY] = py
            geo[at, PZ] = pz
            geo[at, RAD] = dist
            geo[at, RINV] = rinv
            geo[at, UM] = part * part
            geo[at, TM] = part
            geo[at, SP] = got[3]
            geo[at, TILE] = tile.astype(f32)
            geo[at, TARGET] = target.astype(f32)
            harmonics(geo, at, px, py, pz)

            acc = [[None] * 4 for _ in range(9)]
            for e in range(E):
                def row(i):
                    return jnp.broadcast_to(geo[at, i, e : e + 1, :], (NB, L))

                diff = row(RAD) - centre
                bump = jnp.exp(-GAMMA * (diff * diff))
                rb = bump * row(UM)
                basis[at, e * 8 : e * 8 + 8, :] = rb
                slope[at, e * 8 : e * 8 + 8, :] = -(bump * row(TM)) - (2.0 * GAMMA) * (diff * rb * row(RINV))
                kind = row(SP)
                per = [jnp.where(kind == float(k), rb, 0.0) for k in range(4)]
                for qm in range(9):
                    y = None if qm == 0 else row(Y1X + qm - 1)
                    for k in range(4):
                        term = per[k] if y is None else y * per[k]
                        acc[qm][k] = term if e == 0 else acc[qm][k] + term
            first = 0
            for q, count in enumerate((1, 3, 5)):
                blocks = []
                for m in range(count):
                    p = jnp.concatenate(acc[first + m], 0)
                    high, low = split2(p)
                    blocks.append(jnp.concatenate([high, low, high], 0))
                first += count
                out = dot(vf_ref[q], jnp.concatenate(blocks, 1) if count > 1 else blocks[0])
                if q == 0:
                    value = out
                else:
                    value = None
                    for m in range(count):
                        a = out[:, m * L : (m + 1) * L]
                        moment[at, (0, 3)[q - 1] + m] = a
                        value = a * a if value is None else value + a * a
                high, low = split2(value)
                inv[q * C : (q + 1) * C, r * L : (r + 1) * L] = high
                inv[384 + q * C : 384 + (q + 1) * C, r * L : (r + 1) * L] = low
                inv[768 + q * C : 768 + (q + 1) * C, r * L : (r + 1) * L] = high
        z = dot(mf_ref[0], inv[...])
        update, slope_z = silu_parts(z)
        kind = jnp.concatenate([jnp.broadcast_to(k, (16, L)) for k in kinds], 1)
        sel = iota((16, 2 * L), 0)
        hot = jnp.where((kind == (sel % 4).astype(f32)) & (sel < 12), 1.0, 0.0).astype(bf16)
        h1 = dot(et_ref[...], hot) + update
        for r in range(2):
            hid[xr * 2 + r] = h1[:, r * L : (r + 1) * L]
            dsilu[xr * 2 + r] = slope_z[:, r * L : (r + 1) * L]
        return 0

    lax.fori_loop(0, 4, layer_one, 0)

    read = ro_ref[...]
    low_half = lanes((C, L)) < 64
    for plane in range(4):
        for r in range(2):
            if plane in (1, 2):
                keep = low_half if r == 1 else ~low_half
                dhid[plane * 2 + r] = jnp.where(keep, read, 0.0)
            else:
                dhid[plane * 2 + r] = jnp.zeros((C, L), f32)

    def layer_two(x, _):
        a, b = (x + 1) * 2, (x + 1) * 2 + 1
        ids = halves(edges[a, 0:16, :], edges[b, 0:16, :]).astype(i32)
        _, _, _, tile, target = decode(ids)
        geo2[TILE] = tile.astype(f32)
        geo2[TARGET] = target.astype(f32)
        for i in (PX, PY, PZ, Y1X, Y1Y, Y1Z, Y20, Y21, Y22, Y23, Y24):
            geo2[i] = halves(geo[a, i], geo[b, i])
        rb2[...] = halves(basis[a], basis[b])
        for e in range(E):
            high, low = split2(rb2[e * 8 : e * 8 + 8, :])
            high = high.astype(f32)
            rbst[:, e * L : (e + 1) * L] = jnp.concatenate([high, low.astype(f32), high], 0).astype(bf16)
        for t in range(6):
            h = hid[(x + t // 2) * 2 + t % 2]
            high, low = split2(h)
            hg[0:128, t * L : (t + 1) * L] = high
            hg[128:256, t * L : (t + 1) * L] = low
        spot = iota((C, L), 0).astype(f32).astype(bf16)
        one, zero = jnp.ones((), bf16), jnp.zeros((), bf16)
        for e in range(E):
            where_t = geo2[TILE, e : e + 1, :]
            where_l = geo2[TARGET, e : e + 1, :]
            for t in range(6):
                code = jnp.where(where_t == float(t), where_l, -1.0).astype(bf16)
                hot = jnp.where(spot == jnp.broadcast_to(code, (C, L)), one, zero)
                onehot[t * L : (t + 1) * L, e * L : (e + 1) * L] = hot

        def gather(i, _):
            at = pl.ds(pl.multiple_of(i * 256, 256), 256)
            out = dot(hg[...], onehot[:, at])
            hs[:, at] = out[0:128] + out[128:256]
            rad2[:, at] = dot(wf_ref[...], rbst[:, at])
            return 0

        lax.fori_loop(0, 8, gather, 0)

        def contract(i, _):
            rows = pl.multiple_of(i * 16, 16)
            acc = [None] * 9
            for e in range(E):
                cols = slice(e * L, (e + 1) * L)
                h = hs[pl.ds(rows, 16), cols]
                ts = [rad2[pl.ds(q * C + rows, 16), cols] * h for q in range(3)]
                for qm in range(9):
                    if qm == 0:
                        term = ts[0]
                    else:
                        y = jnp.broadcast_to(geo2[Y1X + qm - 1, e : e + 1, :], (16, L))
                        term = y * ts[1 if qm < 4 else 2]
                    acc[qm] = term if e == 0 else acc[qm] + term
            for qm in range(9):
                efac[qm, pl.ds(rows, 16), :] = acc[qm] * SCALE
            return 0

        lax.fori_loop(0, 8, contract, 0)

        one_sq = efac[1] * efac[1] + efac[2] * efac[2] + efac[3] * efac[3]
        two_sq = efac[4] * efac[4]
        for m in range(5, 9):
            two_sq = two_sq + efac[m] * efac[m]
        for q, value in enumerate((efac[0], one_sq, two_sq)):
            high, low = split2(value)
            inv[q * C : (q + 1) * C, 0:128] = high
            inv[384 + q * C : 384 + (q + 1) * C, 0:128] = low
            inv[768 + q * C : 768 + (q + 1) * C, 0:128] = high
        z = dot(mf_ref[1], inv[:, 0:128])
        update, slope_z = silu_parts(z)
        h2 = halves(hid[a], hid[b]) + update
        kind = table[(x + 2) * 3 + 1, 3:4, :]
        offset = jnp.zeros((1, L), f32)
        for k in range(4):
            offset = jnp.where(kind == float(k), eo_ref[k : k + 1, :], offset)
        energy = jnp.sum(read * h2, 0, keepdims=True) + offset
        geo2[RAD, 0:1, :] = energy
        extra[x, 0, 0, 0:1, :] = energy

        high, low = split2(read * slope_z)
        dinv = dot(mb_ref[1], jnp.concatenate([high, low, high], 0))
        efac[0] = dinv[0:128] * SCALE
        for m in range(1, 9):
            part = dinv[128:256] if m < 4 else dinv[256:384]
            efac[m] = efac[m] * part * (2.0 * SCALE)

        def back(e, _):
            cols = pl.ds(pl.multiple_of(e * L, L), L)

            def row(i):
                return jnp.broadcast_to(geo2[i, pl.ds(e, 1), :], (16, L))

            ys = [None] + [row(Y1X + m) for m in range(8)]
            acc = [None] * 9
            for i in range(8):
                rows = slice(i * 16, i * 16 + 16)
                h = hs[rows, cols]
                rr = [rad2[q * C + i * 16 : q * C + i * 16 + 16, cols] for q in range(3)]
                ef = [efac[qm, rows, :] for qm in range(9)]
                d0 = ef[0]
                d1 = ys[1] * ef[1] + ys[2] * ef[2] + ys[3] * ef[3]
                d2 = ys[4] * ef[4] + ys[5] * ef[5] + ys[6] * ef[6] + ys[7] * ef[7] + ys[8] * ef[8]
                t1 = rr[1] * h
                t2 = rr[2] * h
                for qm in range(1, 9):
                    term = (t1 if qm < 4 else t2) * ef[qm]
                    acc[qm] = term if i == 0 else acc[qm] + term
                high, low = split2(d0 * rr[0] + d1 * rr[1] + d2 * rr[2])
                dhs[rows, cols] = high
                dhs[128 + i * 16 : 144 + i * 16, cols] = low
                for q, d in enumerate((d0, d1, d2)):
                    high, low = split2(d * h)
                    drad[q, rows, cols] = high
                    drad[q, 128 + i * 16 : 144 + i * 16, cols] = low
            fold = [None] + [acc[m][0:8] + acc[m][8:16] for m in range(1, 9)]
            px, py, pz = (jnp.broadcast_to(geo2[i, pl.ds(e, 1), :], (8, L)) for i in (PX, PY, PZ))
            gx = R3 * fold[1] + R15 * (py * fold[4] + pz * fold[7] + px * fold[8]) - R5 * (px * fold[6])
            gy = R3 * fold[2] + R15 * (px * fold[4] + pz * fold[5] - py * fold[8]) - R5 * (py * fold[6])
            gz = R3 * fold[3] + R15 * (py * fold[5] + px * fold[7]) + (2.0 * R5) * (pz * fold[6])
            extra[x, e + 1, 1] = roll(0.5 * gx, 64)
            extra[x, e + 1, 2] = roll(0.5 * gy, 64)
            extra[x, e + 1, 3] = roll(0.5 * gz, 64)
            return 0

        lax.fori_loop(0, E, back, 0)

        grad = dot(wb_ref[0], drad[0]) + dot(wb_ref[1], drad[1]) + dot(wb_ref[2], drad[2])
        for e in range(E):
            g = grad[0:8, e * L : (e + 1) * L] + grad[8:16, e * L : (e + 1) * L]
            extra[x, e + 1, 0] = roll(g, 64)
        for t in range(6):
            out = dot(dhs[...], onehot[t * L : (t + 1) * L, :], ((1,), (1,)))
            at = (x + t // 2) * 2 + t % 2
            dhid[at] = dhid[at] + (out[0:128] + out[128:256])
        return 0

    lax.fori_loop(0, 2, layer_two, 0)

    for i in range(18):
        force[i] = jnp.zeros((8, L), f32)
    sub8 = iota((8, L), 0)
    spot = iota((C, L), 0).astype(f32).astype(bf16)
    one, zero = jnp.ones((), bf16), jnp.zeros((), bf16)

    def layer_one_back(xr, _):
        inner = (xr == 1) | (xr == 2)
        x_own = jnp.clip(xr - 1, 0, 1)
        dz = jnp.concatenate([dhid[xr * 2 + r] * dsilu[xr * 2 + r] for r in range(2)], 1)
        high, low = split2(dz)
        dinv = dot(mb_ref[0], jnp.concatenate([high, low, high], 0))
        for r in range(2):
            at = xr * 2 + r
            cols = slice(r * L, (r + 1) * L)
            first = 0
            for q, count in enumerate((1, 3, 5)):
                part = dinv[q * C : (q + 1) * C, cols]
                blocks = []
                for m in range(count):
                    da = part if q == 0 else 2.0 * moment[at, (0, 3)[q - 1] + m] * part
                    high, low = split2(da)
                    blocks.append(jnp.concatenate([high, low], 0))
                out = dot(vb_ref[q], jnp.concatenate(blocks, 1) if count > 1 else blocks[0])
                for m in range(count):
                    one_m = out[:, m * L : (m + 1) * L]
                    dmom[first + m] = one_m[0:32] + one_m[32:64]
                first += count
            keep = ((lane8 >= 64) if r == 0 else (lane8 < 64)) & inner
            received = jnp.zeros((8, L), f32)
            for e in range(E):
                def row(i):
                    return jnp.broadcast_to(geo[at, i, e : e + 1, :], (NB, L))

                kind = row(SP)
                is0, is1, is2 = kind == 0.0, kind == 1.0, kind == 2.0
                dp = []
                for qm in range(9):
                    sel = jnp.where(is2, dmom[qm, 16:24, :], dmom[qm, 24:32, :])
                    sel = jnp.where(is1, dmom[qm, 8:16, :], sel)
                    dp.append(jnp.where(is0, dmom[qm, 0:8, :], sel))
                rb = basis[at, e * 8 : e * 8 + 8, :]
                g = dp[0]
                for m in range(8):
                    g = g + row(Y1X + m) * dp[m + 1]
                g = g + jnp.where(keep, extra[x_own, e + 1, 0], 0.0)
                radial = (2.0 * g) * slope[at, e * 8 : e * 8 + 8, :]
                px, py, pz = row(PX), row(PY), row(PZ)
                c22 = dp[6] * (1.0 / R3)
                half = (0.5 * R15) * rb
                hr = (0.5 * R3) * rb
                gx = px * radial + hr * dp[1] + half * (py * dp[4] + pz * dp[7] + px * (dp[8] - c22))
                gy = py * radial + hr * dp[2] + half * (px * dp[4] + pz * dp[5] - py * (dp[8] + c22))
                gz = pz * radial + hr * dp[3] + half * (py * dp[5] + px * dp[7] + pz * (c22 + c22))
                gx = gx + jnp.where(keep, extra[x_own, e + 1, 1], 0.0)
                gy = gy + jnp.where(keep, extra[x_own, e + 1, 2], 0.0)
                gz = gz + jnp.where(keep, extra[x_own, e + 1, 3], 0.0)
                sx = jnp.sum(gx, 0, keepdims=True)
                sy = jnp.sum(gy, 0, keepdims=True)
                sz = jnp.sum(gz, 0, keepdims=True)
                vec = jnp.where(sub8 == 0, sx, jnp.where(sub8 == 1, sy, jnp.where(sub8 == 2, sz, 0.0)))
                received = received + vec
                high, low = split2(vec)
                both = jnp.concatenate([high.astype(f32), low.astype(f32)], 0)
                where_t = jnp.broadcast_to(geo[at, TILE, e : e + 1, :], (16, L))
                for t in range(6):
                    pick[t * 16 : (t + 1) * 16, e * L : (e + 1) * L] = jnp.where(
                        where_t == float(t), both, 0.0
                    ).astype(bf16)
                code = jnp.broadcast_to(geo[at, TARGET, e : e + 1, :].astype(bf16), (C, L))
                onehot[0:128, e * L : (e + 1) * L] = jnp.where(spot == code, one, zero)
            sent = dot(pick[...], onehot[0:128, :], ((1,), (1,)))
            for t in range(6):
                to = (xr + t // 2) * 3 + r + t % 2
                force[to] = force[to] - (sent[t * 16 : t * 16 + 8] + sent[t * 16 + 8 : t * 16 + 16])
            turned = roll(received, 64)
            mine = (xr + 1) * 3 + r
            force[mine] = force[mine] + jnp.where(lane8 >= 64, turned, 0.0)
            force[mine + 1] = force[mine + 1] + jnp.where(lane8 < 64, turned, 0.0)
        return 0

    lax.fori_loop(0, 4, layer_one_back, 0)

    for plane in range(6):
        for pair in range(3):
            out = (outl_ref, outo_ref, outr_ref)[plane // 2]
            at = ((plane % 2) * 3 + pair) * 4
            out[at : at + 4, :] = force[plane * 3 + pair, 0:4, :]
            if plane in (2, 3) and pair == 1:
                out[at + 3 : at + 4, :] = extra[plane - 2, 0, 0, 0:1, :]


def chunk_kernel(gy_ref, gz_ref, own_ref, left_ref, right_ref, out_ref):
    gy, gz = gy_ref[0], gz_ref[0]
    front = gz == 0
    total = own_ref[...] + left_ref[...] + right_ref[...]
    quarter = lanes((4, L)) // 32

    def squeeze(pair, zh):
        first = total[pair * 4 : pair * 4 + 4]
        second = total[12 + pair * 4 : 16 + pair * 4]
        out = roll(first, -32 * zh)
        out = jnp.where(quarter == 1, roll(first, -32 - 32 * zh), out)
        out = jnp.where(quarter == 2, roll(second, 64 - 32 * zh), out)
        return jnp.where(quarter == 3, roll(second, 32 - 32 * zh), out)

    out_ref[...] = jnp.zeros(out_ref.shape, f32)
    y_count = out_ref.shape[0] // 2
    beside = jnp.where(front, gy + y_count - 1, gy + 1)
    beside = jnp.where(beside >= y_count, beside - y_count, beside)
    for zh in range(2):
        parts = [squeeze(pair, zh) for pair in range(3)]
        low = jnp.where(front, parts[1], parts[0])
        high = jnp.where(front, parts[2], parts[1])
        near = jnp.where(front, parts[0], parts[2])
        out_ref[gy * 2 + zh] = jnp.concatenate([low, high], 0)
        out_ref[beside * 2 + zh, 0:4, :] = near


def unpack_kernel(gy_ref, got_ref, energy_ref, force_ref):
    gy = gy_ref[0]
    y_count = got_ref.shape[0] // 2
    below = jnp.where(gy == 0, y_count - 1, gy - 1)
    above = jnp.where(gy == y_count - 1, 0, gy + 1)
    own = got_ref[gy * 2] + got_ref[gy * 2 + 1]
    low = own[0:4] + got_ref[below * 2 + 1, 0:4, :]
    high = own[4:8] + got_ref[above * 2, 0:4, :]
    lower = lanes((4, L)) < 64
    first = jnp.where(lower, low, roll(high, 64))
    second = jnp.where(lower, roll(low, 64), high)
    rows = jnp.concatenate([first, second], 1)
    keep, spread8 = block_masks(3)
    group = jnp.where((iota((96, 8), 0) // 4) % 3 == iota((96, 8), 1), 1.0, 0.0).astype(bf16)
    rows8 = jnp.concatenate([rows, jnp.zeros((4, 256), f32)], 0)
    nt = ((1,), (1,))
    total = None
    for part in split3(rows8):
        wide = jnp.where(keep, dot(group, part), 0.0).astype(bf16)
        piece = dot(wide, spread8, nt)
        total = piece if total is None else total + piece
    force_ref[...] = total
    keep, _ = block_masks(1)
    total = None
    for part in split3(rows[3:4]):
        wide = jnp.where(keep, part.astype(f32), 0.0).astype(bf16)
        piece = dot(wide, spread8, nt)
        total = piece if total is None else total + piece
    energy_ref[...] = total


def call(kernel, outs, in_specs, scratch=(), flops=10**6, vmem=4):
    return pl.pallas_call(
        kernel,
        out_shape=outs,
        in_specs=in_specs,
        out_specs=jax.tree.map(lambda _: pl.BlockSpec(memory_space=VMEM), outs),
        scratch_shapes=list(scratch),
        compiler_params=pltpu.CompilerParams(vmem_limit_bytes=int(vmem * 2**20)),
        cost_estimate=pl.CostEstimate(flops=flops, bytes_accessed=10**5, transcendentals=0),
    )


def shape(*dims, dtype=f32):
    return jax.ShapeDtypeStruct(dims, dtype)


def shards(
    positions, species, neighbors, edge_mask, species_embed, radial_weight, mix_weight, readout, energy_offset
):
    v = pl.BlockSpec(memory_space=VMEM)
    sm = pl.BlockSpec(memory_space=SMEM)
    gy_count, gz_count = lax.axis_size("gy"), lax.axis_size("gz")
    gx_count = lax.axis_size("gx")
    gy, gz = lax.axis_index("gy"), lax.axis_index("gz")
    gy_only = gy.astype(i32).reshape(1)
    gz_only = gz.astype(i32).reshape(1)

    own, straight, cross = call(
        pack_kernel,
        [shape(40, 256), shape(40, L), shape(40, L)],
        [sm] + [pl.BlockSpec(memory_space=pltpu.HBM)] * 4,
        [VMEM((96, 8), f32), VMEM((32, 8), i32), VMEM((256, E), i32), VMEM((256, E), i32), pltpu.SemaphoreType.DMA((4,))],
        vmem=53.8,
    )(
        gz_only,
        positions.transpose(0, 1, 4, 2, 3).reshape(96, 8),
        species.reshape(32, 8),
        neighbors.reshape(256, E),
        edge_mask.reshape(256, E),
    )

    def dev(y, s):
        return (y % gy_count) * gz_count + s

    yz = ("gy", "gz")
    go_straight = [(dev(y, s), dev(y + 1 if s == 0 else y - 1, s)) for y in range(gy_count) for s in range(2)]
    go_cross = [(dev(y, s), dev(y - 1 if s == 0 else y + 1, 1 - s)) for y in range(gy_count) for s in range(2)]
    near_straight = lax.ppermute(straight, yz, go_straight)
    near_cross = lax.ppermute(cross, yz, go_cross)
    both = lax.all_gather(own, "gz")

    left, right = call(rows_kernel, [shape(88, L), shape(88, L)], [sm, v, v, v])(
        gz_only, both, near_straight, near_cross
    )
    up = [(i, (i + 1) % gx_count) for i in range(gx_count)]
    down = [(j, i) for i, j in up]
    from_left = lax.ppermute(right, "gx", up)
    from_right = lax.ppermute(left, "gx", down)

    weights = call(
        weights_kernel,
        [
            shape(3, C, 96, dtype=bf16),
            shape(3, 64, 256, dtype=bf16),
            shape(384, 24, dtype=bf16),
            shape(3, 16, 256, dtype=bf16),
            shape(2, C, 1152, dtype=bf16),
            shape(2, 384, 384, dtype=bf16),
            shape(C, 16, dtype=bf16),
            shape(C, L),
            shape(4, L),
        ],
        [v] * 5,
        flops=10**7,
        vmem=8,
    )(species_embed, radial_weight, mix_weight, readout.reshape(1, C), energy_offset.reshape(1, 4))

    scratch = [
        VMEM((18, 8, L), f32),
        VMEM((8, 32, L), f32),
        VMEM((8, 18, E, L), f32),
        VMEM((8, 128, L), f32),
        VMEM((8, 128, L), f32),
        VMEM((8, 8, C, L), f32),
        VMEM((8, C, L), f32),
        VMEM((8, C, L), f32),
        VMEM((8, C, L), f32),
        VMEM((9, 32, L), f32),
        VMEM((1152, 256), bf16),
        VMEM((18, E, L), f32),
        VMEM((128, L), f32),
        VMEM((24, E * L), bf16),
        VMEM((256, 768), bf16),
        VMEM((768, E * L), bf16),
        VMEM((C, E * L), f32),
        VMEM((384, E * L), f32),
        VMEM((9, C, L), f32),
        VMEM((256, E * L), bf16),
        VMEM((3, 256, E * L), bf16),
        VMEM((2, E + 1, 4, 8, L), f32),
        VMEM((96, E * L), bf16),
        VMEM((18, 8, L), f32),
    ]
    out_left, out_own, out_right = call(
        main_kernel, [shape(24, L)] * 3, [v] * 13, scratch, flops=10**9, vmem=48
    )(left, right, from_left, from_right, *weights)

    back_right = lax.ppermute(out_left, "gx", down)
    back_left = lax.ppermute(out_right, "gx", up)
    chunks = call(chunk_kernel, shape(gy_count * 2, 8, L), [sm, sm, v, v, v])(gy_only, gz_only, out_own, back_left, back_right)
    got = lax.all_to_all(chunks, yz, 0, 0)
    energy, force = call(unpack_kernel, [shape(32, 8), shape(96, 8)], [sm, v])(gy_only, got)
    return energy.reshape(2, 4, 4, 8), force.reshape(2, 4, 3, 4, 8).transpose(0, 1, 3, 4, 2)


def solution(mesh):
    in_specs = (
        P("gx", "gy", "gz", None, None),
        P("gx", "gy", "gz", None),
        P("gx", "gy", "gz", None, None),
        P("gx", "gy", "gz", None, None),
        P(),
        P(),
        P(),
        P(),
        P(),
    )
    out_specs = (P("gx", "gy", "gz", None), P("gx", "gy", "gz", None, None))
    return jax.shard_map(shards, mesh=mesh, in_specs=in_specs, out_specs=out_specs, check_vma=False)
```

```python
import math

import jax
import jax.numpy as jnp
from jax import lax
from jax.experimental import pallas as pl
from jax.experimental.pallas import tpu as pltpu
from jax.sharding import PartitionSpec as P

f32 = jnp.float32
bf16 = jnp.bfloat16
i32 = jnp.int32

E = 16
C = 128
NB = 8
L = 128
CUT = 2.0
GAMMA = ((NB - 1) / CUT) ** 2
SCALE = E**-0.5
R3 = math.sqrt(3.0)
R5 = math.sqrt(5.0)
R15 = math.sqrt(15.0)
VMEM = pltpu.VMEM
SMEM = pltpu.SMEM


def split2(x):
    return x, x - x.astype(bf16).astype(f32)


def split3(x):
    high = x.astype(bf16)
    rest = x - high.astype(f32)
    mid = rest.astype(bf16)
    low = (rest - mid.astype(f32)).astype(bf16)
    return high, mid, low


def dot(a, b, dims=((1,), (0,))):
    return lax.dot_general(a, b, (dims, ((), ())), preferred_element_type=f32)


def iota(shape, dim):
    return lax.broadcasted_iota(i32, shape, dim)


def roll(x, shift):
    return pltpu.roll(x, shift % x.shape[-1], x.ndim - 1)


def lanes(shape):
    return iota(shape, len(shape) - 1)


def block_masks(count):
    row, lane = iota((32 * count, 256), 0), iota((32 * count, 256), 1)
    keep = (lane // 32 == row // (4 * count)) & ((lane // 8) % 4 == row % 4)
    spread8 = jnp.where(iota((8, 256), 1) % 8 == iota((8, 256), 0), 1.0, 0.0).astype(bf16)
    return keep, spread8


def pack_kernel(
    gz_ref, pos_hbm, spec_hbm, nbr_hbm, mask_hbm, own_ref, straight_ref, cross_ref, pos_ref, spec_ref, nbr_ref, mask_ref, sems
):
    copies = [
        pltpu.make_async_copy(src, dst, sems.at[i])
        for i, (src, dst) in enumerate(
            ((nbr_hbm, nbr_ref), (mask_hbm, mask_ref), (pos_hbm, pos_ref), (spec_hbm, spec_ref))
        )
    ]
    for copy in copies:
        copy.start()
    for copy in copies:
        copy.wait()
    eye16 = jnp.where(iota((E, E), 0) == iota((E, E), 1), 1.0, 0.0).astype(bf16)
    own_ref[0:16, :] = dot(eye16, nbr_ref[...].astype(f32).astype(bf16), ((1,), (1,)))
    own_ref[16:32, :] = dot(eye16, mask_ref[...].astype(f32).astype(bf16), ((1,), (1,)))
    keep, spread8 = block_masks(3)
    group = jnp.where((iota((8, 96), 1) // 4) % 3 == iota((8, 96), 0), 1.0, 0.0).astype(bf16)
    tail = None
    for part in split3(pos_ref[...]):
        rows = jnp.where(keep, dot(part, spread8), 0.0).astype(bf16)
        piece = dot(group, rows)
        tail = piece if tail is None else tail + piece
    keep, _ = block_masks(1)
    kinds = jnp.where(keep, dot(spec_ref[...].astype(f32).astype(bf16), spread8), 0.0)
    species = jnp.sum(kinds, 0, keepdims=True)
    own_ref[32:40, :] = jnp.where(iota((8, 256), 0) == 3, species, tail)

    lower = lanes((40, L)) < 64
    first, second = own_ref[:, 0:128], own_ref[:, 128:256]
    rows_low = jnp.where(lower, first, roll(second, 64))
    rows_high = jnp.where(lower, roll(first, 64), second)
    front = gz_ref[0] == 0
    straight_ref[...] = jnp.where(front, rows_high, rows_low)
    cross_ref[...] = jnp.where(front, rows_low, rows_high)


def spread(half0, half1, start):
    quarter = lanes((40, L)) // 32
    out = roll(half0, -start)
    out = jnp.where(quarter == 1, roll(half1, 32 - start), out)
    out = jnp.where(quarter == 2, roll(half0, 32 - start), out)
    return jnp.where(quarter == 3, roll(half1, 64 - start), out)


def halves(first, second):
    return roll(jnp.where(lanes(first.shape) >= 64, first, second), 64)


def rows_kernel(gz_ref, all_ref, straight_ref, cross_ref, left_ref, right_ref):
    front = gz_ref[0] == 0
    near0 = jnp.where(front, straight_ref[...], cross_ref[...])
    near1 = jnp.where(front, cross_ref[...], straight_ref[...])
    for x in range(2):
        near = spread(near0, near1, 64 * x)
        own = [
            spread(all_ref[0, :, x * L : (x + 1) * L], all_ref[1, :, x * L : (x + 1) * L], 64 * pair)
            for pair in range(2)
        ]
        tiles = [
            jnp.where(front, near, own[0]),
            jnp.where(front, own[0], own[1]),
            jnp.where(front, own[1], near),
        ]
        for pair in range(3):
            at = (x * 3 + pair) * 4
            left_ref[at : at + 4, :] = tiles[pair][32:36]
            right_ref[at : at + 4, :] = tiles[pair][32:36]
        out = left_ref if x == 0 else right_ref
        for r in range(2):
            out[24 + 32 * r : 56 + 32 * r, :] = halves(tiles[r][0:32], tiles[r + 1][0:32])


def weights_kernel(
    emb_ref, rad_ref, mix_ref, read_ref, off_ref, vf_ref, vb_ref, wf_ref, wb_ref, mf_ref, mb_ref, et_ref, ro_ref, eo_ref
):
    emb = emb_ref[...]
    for q in range(3):
        base = rad_ref[0, :, q * C : (q + 1) * C] * SCALE
        v = jnp.concatenate([base * emb[k : k + 1] for k in range(4)], 0)
        high, low = split2(v)
        vb_ref[q, 0:32, 0:128] = high
        vb_ref[q, 0:32, 128:256] = high
        vb_ref[q, 32:64, 0:128] = low
        vb_ref[q, 32:64, 128:256] = jnp.zeros((32, 128), f32)
        high, low = split2(v.T)
        vf_ref[q] = jnp.concatenate([high, high, low], 1)
        w = rad_ref[1, :, q * C : (q + 1) * C]
        both = jnp.concatenate(split2(w), 0)
        wb_ref[q, :, 0:128] = both
        wb_ref[q, :, 128:256] = jnp.where(iota((16, 128), 0) < 8, both, 0.0)
        high, low = split2(w.T)
        wf_ref[q] = jnp.concatenate([high, high, low], 1)
    for layer in range(2):
        for q in range(3):
            m = mix_ref[layer, q * C : (q + 1) * C, :]
            high, low = split2(m)
            mb_ref[layer, q * C : (q + 1) * C, 0:128] = high
            mb_ref[layer, q * C : (q + 1) * C, 128:256] = high
            mb_ref[layer, q * C : (q + 1) * C, 256:384] = low
            high, low = split2(m.T)
            mf_ref[layer, :, q * C : (q + 1) * C] = high
            mf_ref[layer, :, 384 + q * C : 384 + (q + 1) * C] = high
            mf_ref[layer, :, 768 + q * C : 768 + (q + 1) * C] = low
    high, mid, low = split3(emb)
    stack = jnp.concatenate([high.astype(f32), mid.astype(f32), low.astype(f32), jnp.zeros((4, C), f32)], 0)
    et_ref[...] = stack.T
    ro_ref[...] = jnp.broadcast_to(read_ref[...], (C, L)).T
    pick = jnp.where(iota((4, 4), 0) == iota((4, 4), 1), off_ref[...], 0.0)
    eo_ref[...] = jnp.broadcast_to(jnp.sum(pick, 1, keepdims=True), (4, L))


def decode(ids):
    cell = ids >> 3
    ox = (cell >= 9).astype(i32) + (cell >= 18).astype(i32)
    rest = cell - 9 * ox
    oy = (rest >= 3).astype(i32) + (rest >= 6).astype(i32)
    oz = rest - 3 * oy
    lane = lanes(ids.shape)
    ys = (lane >> 6) + oy
    zs = ((lane >> 3) + oz + 7) & 7
    tile = ox * 2 + (ys >> 1)
    target = ((ys & 1) << 6) | (zs << 3) | (ids & 7)
    return ox, oy, oz, tile, target


PX, PY, PZ, RAD, RINV, UM, TM, SP, TILE, TARGET, Y1X, Y1Y, Y1Z, Y20, Y21, Y22, Y23, Y24 = range(18)
COUNTS = (1, 3, 5)
HALF = (1.0,) + (0.5 * R3,) * 3 + (0.5 * R15, 0.5 * R15, 0.5 * R5, 0.5 * R15, 0.5 * R15)


def silu_parts(v):
    gate = 1.0 / (1.0 + jnp.exp(-v))
    return v * gate, gate * (1.0 + v * (1.0 - gate))


def order_of(qm):
    return 0 if qm == 0 else 1 if qm < 4 else 2


def one_hot_block(code16, block):
    spot = (iota((16, L), 0) + 16 * block).astype(f32).astype(bf16)
    return jnp.where(spot == code16, jnp.ones((), bf16), jnp.zeros((), bf16))


def main_kernel(
    lown_ref, rown_ref, froml_ref, fromr_ref,
    vf_ref, vb_ref, wf_ref, wb_ref, mf_ref, mb_ref, et_ref, ro_ref, eo_ref,
    outl_ref, outo_ref, outr_ref,
    table, edges, geo, basis, slope, psplit, moment, zbuf, inv, hid, dsilu, dhid, dmom, geo2,
    rbst, hg, hs, rad2, efac, invx, dha, dhb, dra, drb, dacc, extra, dsplit, force, energy,
):
    for plane, (ref, base) in enumerate(
        ((froml_ref, 0), (froml_ref, 1), (lown_ref, 0), (lown_ref, 1), (fromr_ref, 0), (fromr_ref, 1))
    ):
        for pair in range(3):
            at = (base * 3 + pair) * 4
            table[plane * 3 + pair, 0:4, :] = ref[at : at + 4, :]
    for plane, ref in enumerate((froml_ref, lown_ref, rown_ref, fromr_ref)):
        for r in range(2):
            edges[plane * 2 + r] = ref[24 + 32 * r : 56 + 32 * r, :]

    centre = iota((NB, L), 0).astype(f32) * (CUT / (NB - 1))

    def sums(xr, r):
        at = xr * 2 + r
        base = (xr + 1) * 3 + r
        own = halves(table[base], table[base + 1])
        ids = edges[at, 0:16, :].astype(i32)
        ox, oy, oz, tile, target = decode(ids)
        got = [jnp.zeros((E, L), f32) for _ in range(4)]
        for t in range(6):
            src = table[(xr + t // 2) * 3 + r + t % 2]
            here = tile == t
            for q in range(4):
                wide = jnp.broadcast_to(src[q : q + 1], (E, L))
                val = jnp.take_along_axis(wide, target, axis=1, mode="promise_in_bounds")
                got[q] = jnp.where(here, val, got[q])
        dx = ((ox - 1).astype(f32) + got[0]) - own[0:1]
        dy = ((oy - 1).astype(f32) + got[1]) - own[1:2]
        dz = ((oz - 1).astype(f32) + got[2]) - own[2:3]
        sq = dx * dx + dy * dy + dz * dz
        dist = jnp.sqrt(sq)
        part = jnp.where(dist < CUT, 1.0 - sq * (1.0 / CUT**2), 0.0) * edges[at, 16:32, :]
        px, py, pz = 0.5 * dx, 0.5 * dy, 0.5 * dz
        geo[at, PX] = px
        geo[at, PY] = py
        geo[at, PZ] = pz
        geo[at, RAD] = dist
        geo[at, RINV] = lax.rsqrt(sq)
        geo[at, UM] = part * part
        geo[at, TM] = part
        geo[at, SP] = got[3]
        geo[at, TILE] = tile.astype(f32)
        geo[at, TARGET] = target.astype(f32)
        geo[at, Y1X] = R3 * px
        geo[at, Y1Y] = R3 * py
        geo[at, Y1Z] = R3 * pz
        geo[at, Y20] = R15 * px * py
        geo[at, Y21] = R15 * py * pz
        geo[at, Y22] = (0.5 * R5) * (2.0 * pz * pz - px * px - py * py)
        geo[at, Y23] = R15 * px * pz
        geo[at, Y24] = (0.5 * R15) * (px * px - py * py)

        def row(i, e):
            return jnp.broadcast_to(geo[at, i, e : e + 1, :], (NB, L))

        for e in range(E):
            diff = row(RAD, e) - centre
            bump = jnp.exp(-GAMMA * (diff * diff))
            rb = bump * row(UM, e)
            basis[at, e] = rb
            slope[at, e] = (-2.0) * (bump * row(TM, e)) - (4.0 * GAMMA) * (diff * rb * row(RINV, e))
        acc = [[None] * 4 for _ in range(9)]
        for e in range(E):
            rb = basis[at, e]
            kind = row(SP, e)
            per = [jnp.where(kind == float(k), rb, 0.0) for k in range(4)]
            for qm in range(9):
                y = None if qm == 0 else row(Y1X + qm - 1, e)
                for k in range(4):
                    term = per[k] if y is None else y * per[k]
                    acc[qm][k] = term if e == 0 else acc[qm][k] + term
        for qm in range(9):
            for k in range(4):
                high, low = split2(acc[qm][k])
                psplit[at, qm, k * 8 : k * 8 + 8] = high
                psplit[at, qm, 32 + k * 8 : 40 + k * 8] = low

    def invariants(source, dest, width, xr):
        for i in range(8):
            rows = slice(i * 16, i * 16 + 16)
            first = 0
            for q, count in enumerate(COUNTS):
                value = source(first, rows)
                if q > 0:
                    value = value * value
                    for m in range(1, count):
                        a = source(first + m, rows)
                        value = value + a * a
                first += count
                for r in range(width):
                    high, low = split2(value[:, r * L : (r + 1) * L])
                    dest[r, q * C + i * 16 : q * C + i * 16 + 16] = high
                    dest[r, 384 + q * C + i * 16 : 384 + q * C + i * 16 + 16] = low

    def features(xr):
        for qm in range(9):
            both = jnp.concatenate([psplit[xr * 2, qm], psplit[xr * 2 + 1, qm]], 1)
            moment[xr, qm] = dot(vf_ref[order_of(qm)], jnp.concatenate([both, both[0:32]], 0))
        invariants(lambda qm, rows: moment[xr, qm, rows, :], inv, 2, xr)
        both = jnp.concatenate([inv[0], inv[1]], 1)
        zbuf[0] = dot(mf_ref[0], jnp.concatenate([both, both[0:384]], 0))
        sel = iota((16, L), 0)
        hots = []
        for r in range(2):
            base = (xr + 1) * 3 + r
            own = halves(table[base], table[base + 1])
            kind = jnp.broadcast_to(own[3:4], (16, L))
            hots.append(jnp.where((kind == (sel % 4).astype(f32)) & (sel < 12), 1.0, 0.0))
        zbuf[1] = dot(et_ref[...], jnp.concatenate(hots, 1))
        for i in range(16):
            rows = slice(i * 8, i * 8 + 8)
            update, slope_z = silu_parts(zbuf[0, rows, :])
            h1 = zbuf[1, rows, :] + update
            hid[xr * 2, rows, :] = h1[:, 0:L]
            hid[xr * 2 + 1, rows, :] = h1[:, L:]
            dsilu[xr, rows, :] = slope_z

    def layer_one(xr, _):
        features(xr)
        sums(xr + 1, 0)
        sums(xr + 1, 1)
        return 0

    sums(0, 0)
    sums(0, 1)
    lax.fori_loop(0, 3, layer_one, 0)
    features(3)

    low_half = lanes((C, L)) < 64
    for plane in range(4):
        for r in range(2):
            if plane in (1, 2):
                keep = low_half if r == 1 else ~low_half
                dhid[plane, :, r * L : (r + 1) * L] = jnp.where(keep, ro_ref[...], 0.0)
            else:
                dhid[plane, :, r * L : (r + 1) * L] = jnp.zeros((C, L), f32)
    for r in range(2):
        for e in range(E):
            for i in range(4):
                extra[0, r, e, i] = jnp.zeros((8, L), f32)
    lane8 = lanes((8, L))

    def layer_two(x, _):
        a, b = (x + 1) * 2, (x + 1) * 2 + 1
        ids = halves(edges[a, 0:16, :], edges[b, 0:16, :]).astype(i32)
        _, _, _, tile, target = decode(ids)
        geo2[TILE] = tile.astype(f32)
        geo2[TARGET] = target.astype(f32)
        for i in (PX, PY, PZ, Y1X, Y1Y, Y1Z, Y20, Y21, Y22, Y23, Y24):
            geo2[i] = halves(geo[a, i], geo[b, i])
        for e in range(E):
            rb = halves(basis[a, e], basis[b, e])
            high, low = split2(rb)
            rbst[e] = jnp.concatenate([high, low, high], 0)

        for t in range(6):
            high, low = split2(hid[(x + t // 2) * 2 + t % 2])
            hg[t, 0:128] = high.astype(bf16)
            hg[t, 128:256] = low.astype(bf16)

        def code_row(i, e):
            return jnp.broadcast_to(geo2[i, pl.ds(e, 1), :], (16, L))

        def hot_blocks(pair, which):
            tiles = [code_row(TILE, 2 * pair + half) for half in range(2)]
            spots = [code_row(TARGET, 2 * pair + half) for half in range(2)]
            blocks = []
            for t in which:
                codes = [jnp.where(tiles[i] == float(t), spots[i], -1.0).astype(bf16) for i in range(2)]
                for block in range(8):
                    blocks.append(jnp.concatenate([one_hot_block(code, block) for code in codes], 1))
            return jnp.concatenate(blocks, 0)

        def gather(pair):
            table_x = jnp.concatenate([hg[t] for t in range(6)], 1)
            out = dot(table_x, hot_blocks(pair, range(6)))
            both = jnp.concatenate([rbst[2 * pair], rbst[2 * pair + 1]], 1)
            for half in range(2):
                cols = slice(half * L, (half + 1) * L)
                hs[2 * pair + half] = out[0:128, cols] + out[128:256, cols]
            for q in range(3):
                rad = dot(wf_ref[q], both)
                rad2[2 * pair, q] = rad[:, 0:L]
                rad2[2 * pair + 1, q] = rad[:, L:]

        def contract(pair):
            for i in range(8):
                rows = slice(i * 16, i * 16 + 16)
                acc = [None if pair == 0 else efac[qm, rows, :] for qm in range(9)]
                for e in (2 * pair, 2 * pair + 1):
                    h = hs[e, rows, :]
                    ts = [rad2[e, q, rows, :] * h for q in range(3)]
                    for qm in range(9):
                        if qm == 0:
                            term = ts[0]
                        else:
                            y = jnp.broadcast_to(geo2[Y1X + qm - 1, e : e + 1, :], (16, L))
                            term = y * ts[order_of(qm)]
                        acc[qm] = term if acc[qm] is None else acc[qm] + term
                for qm in range(9):
                    efac[qm, rows, :] = acc[qm] * SCALE if pair == 7 else acc[qm]

        gather(0)
        for pair in range(8):
            if pair < 7:
                gather(pair + 1)
            contract(pair)

        invariants(lambda qm, rows: efac[qm, rows, :], invx, 1, 0)
        zbuf[0, :, 0:L] = dot(mf_ref[1], jnp.concatenate([invx[0], invx[0, 0:384]], 0))
        total = jnp.zeros((8, L), f32)
        for i in range(8):
            rows = slice(i * 16, i * 16 + 16)
            update, slope_z = silu_parts(zbuf[0, rows, 0:L])
            term = ro_ref[rows, :] * (halves(hid[a, rows, :], hid[b, rows, :]) + update)
            total = total + (term[0:8] + term[8:16])
            high, low = split2(ro_ref[rows, :] * slope_z)
            invx[0, i * 16 : i * 16 + 16] = high
            invx[0, 128 + i * 16 : 144 + i * 16] = low
        kind = table[(x + 2) * 3 + 1, 3:4, :]
        offset = jnp.zeros((1, L), f32)
        for k in range(4):
            offset = jnp.where(kind == float(k), eo_ref[k : k + 1, :], offset)
        energy[x] = jnp.broadcast_to(jnp.sum(total, 0, keepdims=True) + offset, (8, L))

        both = jnp.concatenate([invx[0, 0:256], invx[0, 0:128]], 0)
        zbuf[0, :, 0:L] = dot(mb_ref[1, 0:128], both)
        zbuf[0, :, L:] = dot(mb_ref[1, 128:256], both)
        zbuf[1, :, 0:L] = dot(mb_ref[1, 256:384], both)
        for i in range(8):
            rows = slice(i * 16, i * 16 + 16)
            efac[0, rows, :] = zbuf[0, rows, 0:L] * SCALE
            one = zbuf[0, rows, L:] * (2.0 * SCALE)
            two = zbuf[1, rows, 0:L] * (2.0 * SCALE)
            for m in range(1, 9):
                efac[m, rows, :] = efac[m, rows, :] * (one if m < 4 else two)

        def edge_grad(e, dh, dr):
            def row(i, n):
                return jnp.broadcast_to(geo2[i, pl.ds(e, 1), :], (n, L))

            ys = [None] + [row(Y1X + m, 16) for m in range(8)]
            acc = [None] * 9
            for i in range(8):
                rows = slice(i * 16, i * 16 + 16)
                low_rows = slice(128 + i * 16, 144 + i * 16)
                h = hs[e, rows, :]
                rr = [rad2[e, q, rows, :] for q in range(3)]
                ef = [efac[qm, rows, :] for qm in range(9)]
                d0 = ef[0]
                d1 = ys[1] * ef[1] + ys[2] * ef[2] + ys[3] * ef[3]
                d2 = ys[4] * ef[4] + ys[5] * ef[5] + ys[6] * ef[6] + ys[7] * ef[7] + ys[8] * ef[8]
                t1 = rr[1] * h
                t2 = rr[2] * h
                for qm in range(1, 9):
                    term = (t1 if qm < 4 else t2) * ef[qm]
                    term = term[0:8] + term[8:16]
                    acc[qm] = term if i == 0 else acc[qm] + term
                dh[rows], dh[low_rows] = split2(d0 * rr[0] + d1 * rr[1] + d2 * rr[2])
                for q, d in enumerate((d0, d1, d2)):
                    dr[q, rows], dr[q, low_rows] = split2(d * h)
            px, py, pz = (row(i, 8) for i in (PX, PY, PZ))
            gx = R3 * acc[1] + R15 * (py * acc[4] + pz * acc[7] + px * acc[8]) - R5 * (px * acc[6])
            gy = R3 * acc[2] + R15 * (px * acc[4] + pz * acc[5] - py * acc[8]) - R5 * (py * acc[6])
            gz = R3 * acc[3] + R15 * (py * acc[5] + px * acc[7]) + (2.0 * R5) * (pz * acc[6])
            for i, g in enumerate((gx, gy, gz)):
                turned = roll(0.5 * g, 64)
                extra[x + 1, 0, e, i + 1] = jnp.where(lane8 >= 64, turned, 0.0)
                extra[x + 1, 1, e, i + 1] = jnp.where(lane8 < 64, turned, 0.0)
        def spread_back(pair, dh, dr):
            grad = None
            for q in range(3):
                piece = dot(wb_ref[q], jnp.concatenate([dr[0, q], dr[1, q]], 1))
                grad = piece if grad is None else grad + piece
            grad = grad[0:8] + grad[8:16]
            for half in range(2):
                turned = roll(grad[:, half * L : (half + 1) * L], 64)
                extra[x + 1, 0, 2 * pair + half, 0] = jnp.where(lane8 >= 64, turned, 0.0)
                extra[x + 1, 1, 2 * pair + half, 0] = jnp.where(lane8 < 64, turned, 0.0)
            left = jnp.concatenate([dh[0], dh[1]], 1).astype(bf16)

            for part in range(3):
                hot = hot_blocks(pair, (2 * part, 2 * part + 1))
                dacc[part] = dacc[part] + dot(left, hot, ((1,), (1,)))

        for part in range(3):
            dacc[part] = jnp.zeros((256, 256), f32)
        for half in range(2):
            edge_grad(half, dhb.at[half], drb.at[half])

        def back(i, _):
            for half in range(2):
                edge_grad(4 * i + 2 + half, dha.at[half], dra.at[half])
            spread_back(2 * i, dhb, drb)
            for half in range(2):
                edge_grad(4 * i + 4 + half, dhb.at[half], drb.at[half])
            spread_back(2 * i + 1, dha, dra)
            return 0

        lax.fori_loop(0, 3, back, 0)
        for half in range(2):
            edge_grad(14 + half, dha.at[half], dra.at[half])
        spread_back(6, dhb, drb)
        spread_back(7, dha, dra)
        for part in range(3):
            for i in range(8):
                rows = slice(i * 16, i * 16 + 16)
                total = dacc[part, rows, :] + dacc[part, 128 + i * 16 : 144 + i * 16, :]
                dhid[x + part, rows, :] = dhid[x + part, rows, :] + total
        return 0

    lax.fori_loop(0, 2, layer_two, 0)

    def sums_back(xr):
        for i in range(8):
            rows = slice(i * 16, i * 16 + 16)
            value = dhid[xr, rows, :] * dsilu[xr, rows, :]
            for r in range(2):
                high, low = split2(value[:, r * L : (r + 1) * L])
                inv[r, i * 16 : i * 16 + 16] = high
                inv[r, 128 + i * 16 : 144 + i * 16] = low
        both = jnp.concatenate([inv[0, 0:256], inv[1, 0:256]], 1)
        both = jnp.concatenate([both, both[0:128]], 0)
        for q in range(3):
            zbuf[q] = dot(mb_ref[0, q * C : (q + 1) * C], both)
        for i in range(8):
            rows = slice(i * 16, i * 16 + 16)
            parts = [zbuf[0, rows, :], 2.0 * zbuf[1, rows, :], 2.0 * zbuf[2, rows, :]]
            for qm in range(9):
                value = parts[0] if qm == 0 else parts[order_of(qm)] * moment[xr, qm, rows, :]
                for r in range(2):
                    high, low = split2(value[:, r * L : (r + 1) * L])
                    dsplit[qm, r, i * 16 : i * 16 + 16] = high
                    dsplit[qm, r, 128 + i * 16 : 144 + i * 16] = low
        for qm in range(9):
            out = dot(vb_ref[order_of(qm)], jnp.concatenate([dsplit[qm, 0], dsplit[qm, 1]], 1))
            out = HALF[qm] * (out[0:32] + out[32:64])
            dmom[xr * 2, qm] = out[:, 0:L]
            dmom[xr * 2 + 1, qm] = out[:, L:]

    for i in range(18):
        force[i] = jnp.zeros((8, L), f32)
    sub8 = iota((8, L), 0)

    def forces(xr):
        slab = xr % 3 if isinstance(xr, int) else jnp.where((xr == 1) | (xr == 2), xr, 0)
        for r in range(2):
            at = xr * 2 + r
            received = jnp.zeros((8, L), f32)
            picks, hots = [], []
            for e in range(E):
                def row(i):
                    return jnp.broadcast_to(geo[at, i, e : e + 1, :], (NB, L))

                kind = row(SP)
                is0, is1, is2 = kind == 0.0, kind == 1.0, kind == 2.0
                dp = []
                for qm in range(9):
                    sel = jnp.where(is2, dmom[at, qm, 16:24, :], dmom[at, qm, 24:32, :])
                    sel = jnp.where(is1, dmom[at, qm, 8:16, :], sel)
                    dp.append(jnp.where(is0, dmom[at, qm, 0:8, :], sel))
                px, py, pz = row(PX), row(PY), row(PZ)
                dz6 = dp[6] * pz
                gx = dp[1] + py * dp[4] + pz * dp[7] + px * (dp[8] - dp[6])
                gy = dp[2] + px * dp[4] + pz * dp[5] - py * (dp[8] + dp[6])
                gz = dp[3] + py * dp[5] + px * dp[7] + (dz6 + dz6)
                g = dp[0] + px * (gx + dp[1]) + py * (gy + dp[2]) + pz * (gz + dp[3])
                g = g + extra[slab, r, e, 0]
                radial = g * slope[at, e]
                rb = basis[at, e]
                gx = px * radial + rb * gx + extra[slab, r, e, 1]
                gy = py * radial + rb * gy + extra[slab, r, e, 2]
                gz = pz * radial + rb * gz + extra[slab, r, e, 3]
                sx = jnp.sum(gx, 0, keepdims=True)
                sy = jnp.sum(gy, 0, keepdims=True)
                sz = jnp.sum(gz, 0, keepdims=True)
                vec = jnp.where(sub8 == 0, sx, jnp.where(sub8 == 1, sy, jnp.where(sub8 == 2, sz, 0.0)))
                received = received + vec
                both = jnp.concatenate(split2(vec), 0).astype(bf16)
                where_t = jnp.broadcast_to(geo[at, TILE, e : e + 1, :], (16, L)).astype(bf16)
                picks.append(
                    [jnp.where(where_t == jnp.full((), t, bf16), both, jnp.zeros((), bf16)) for t in range(6)]
                )
                code = jnp.broadcast_to(geo[at, TARGET, e : e + 1, :], (16, L)).astype(bf16)
                hots.append([one_hot_block(code, block) for block in range(8)])
                if e % 2:
                    left = jnp.concatenate([jnp.concatenate(p, 0) for p in picks], 1)
                    right = jnp.concatenate([jnp.concatenate(h, 0) for h in hots], 1)
                    piece = dot(left, right, ((1,), (1,)))
                    sent = piece if e == 1 else sent + piece
                    picks, hots = [], []
            for t in range(6):
                to = (xr + t // 2) * 3 + r + t % 2
                force[to] = force[to] - (sent[t * 16 : t * 16 + 8] + sent[t * 16 + 8 : t * 16 + 16])
            turned = roll(received, 64)
            mine = (xr + 1) * 3 + r
            force[mine] = force[mine] + jnp.where(lane8 >= 64, turned, 0.0)
            force[mine + 1] = force[mine + 1] + jnp.where(lane8 < 64, turned, 0.0)

    def layer_one_back(xr, _):
        sums_back(xr + 1)
        forces(xr)
        return 0

    sums_back(0)
    lax.fori_loop(0, 3, layer_one_back, 0)
    forces(3)

    for plane in range(6):
        for pair in range(3):
            out = (outl_ref, outo_ref, outr_ref)[plane // 2]
            at = ((plane % 2) * 3 + pair) * 4
            out[at : at + 4, :] = force[plane * 3 + pair, 0:4, :]
            if plane in (2, 3) and pair == 1:
                out[at + 3 : at + 4, :] = energy[plane - 2, 0:1, :]


def chunk_kernel(gy_ref, gz_ref, own_ref, left_ref, right_ref, out_ref):
    gy, gz = gy_ref[0], gz_ref[0]
    front = gz == 0
    total = own_ref[...] + left_ref[...] + right_ref[...]
    quarter = lanes((4, L)) // 32

    def squeeze(pair, zh):
        first = total[pair * 4 : pair * 4 + 4]
        second = total[12 + pair * 4 : 16 + pair * 4]
        out = roll(first, -32 * zh)
        out = jnp.where(quarter == 1, roll(first, -32 - 32 * zh), out)
        out = jnp.where(quarter == 2, roll(second, 64 - 32 * zh), out)
        return jnp.where(quarter == 3, roll(second, 32 - 32 * zh), out)

    out_ref[...] = jnp.zeros(out_ref.shape, f32)
    y_count = out_ref.shape[0] // 2
    beside = jnp.where(front, gy + y_count - 1, gy + 1)
    beside = jnp.where(beside >= y_count, beside - y_count, beside)
    for zh in range(2):
        parts = [squeeze(pair, zh) for pair in range(3)]
        low = jnp.where(front, parts[1], parts[0])
        high = jnp.where(front, parts[2], parts[1])
        near = jnp.where(front, parts[0], parts[2])
        out_ref[gy * 2 + zh] = jnp.concatenate([low, high], 0)
        out_ref[beside * 2 + zh, 0:4, :] = near


def unpack_kernel(gy_ref, got_ref, energy_ref, force_ref):
    gy = gy_ref[0]
    y_count = got_ref.shape[0] // 2
    below = jnp.where(gy == 0, y_count - 1, gy - 1)
    above = jnp.where(gy == y_count - 1, 0, gy + 1)
    own = got_ref[gy * 2] + got_ref[gy * 2 + 1]
    low = own[0:4] + got_ref[below * 2 + 1, 0:4, :]
    high = own[4:8] + got_ref[above * 2, 0:4, :]
    lower = lanes((4, L)) < 64
    first = jnp.where(lower, low, roll(high, 64))
    second = jnp.where(lower, roll(low, 64), high)
    rows = jnp.concatenate([first, second], 1)
    keep, spread8 = block_masks(3)
    group = jnp.where((iota((96, 8), 0) // 4) % 3 == iota((96, 8), 1), 1.0, 0.0).astype(bf16)
    rows8 = jnp.concatenate([rows, jnp.zeros((4, 256), f32)], 0)
    nt = ((1,), (1,))
    total = None
    for part in split3(rows8):
        wide = jnp.where(keep, dot(group, part), 0.0).astype(bf16)
        piece = dot(wide, spread8, nt)
        total = piece if total is None else total + piece
    force_ref[...] = total
    keep, _ = block_masks(1)
    total = None
    for part in split3(rows[3:4]):
        wide = jnp.where(keep, part.astype(f32), 0.0).astype(bf16)
        piece = dot(wide, spread8, nt)
        total = piece if total is None else total + piece
    energy_ref[...] = total


def call(kernel, outs, in_specs, scratch=(), flops=10**6, vmem=4):
    return pl.pallas_call(
        kernel,
        out_shape=outs,
        in_specs=in_specs,
        out_specs=jax.tree.map(lambda _: pl.BlockSpec(memory_space=VMEM), outs),
        scratch_shapes=list(scratch),
        compiler_params=pltpu.CompilerParams(vmem_limit_bytes=int(vmem * 2**20)),
        cost_estimate=pl.CostEstimate(flops=flops, bytes_accessed=10**5, transcendentals=0),
    )


def shape(*dims, dtype=f32):
    return jax.ShapeDtypeStruct(dims, dtype)


def shards(
    positions, species, neighbors, edge_mask, species_embed, radial_weight, mix_weight, readout, energy_offset
):
    v = pl.BlockSpec(memory_space=VMEM)
    sm = pl.BlockSpec(memory_space=SMEM)
    gy_count, gz_count = lax.axis_size("gy"), lax.axis_size("gz")
    gx_count = lax.axis_size("gx")
    gy, gz = lax.axis_index("gy"), lax.axis_index("gz")
    gy_only = gy.astype(i32).reshape(1)
    gz_only = gz.astype(i32).reshape(1)

    own, straight, cross = call(
        pack_kernel,
        [shape(40, 256), shape(40, L), shape(40, L)],
        [sm] + [pl.BlockSpec(memory_space=pltpu.HBM)] * 4,
        [VMEM((96, 8), f32), VMEM((32, 8), i32), VMEM((256, E), i32), VMEM((256, E), i32), pltpu.SemaphoreType.DMA((4,))],
        vmem=53.8,
    )(
        gz_only,
        positions.transpose(0, 1, 4, 2, 3).reshape(96, 8),
        species.reshape(32, 8),
        neighbors.reshape(256, E),
        edge_mask.reshape(256, E),
    )

    def dev(y, s):
        return (y % gy_count) * gz_count + s

    yz = ("gy", "gz")
    go_straight = [(dev(y, s), dev(y + 1 if s == 0 else y - 1, s)) for y in range(gy_count) for s in range(2)]
    go_cross = [(dev(y, s), dev(y - 1 if s == 0 else y + 1, 1 - s)) for y in range(gy_count) for s in range(2)]
    near_straight = lax.ppermute(straight, yz, go_straight)
    near_cross = lax.ppermute(cross, yz, go_cross)
    both = lax.all_gather(own, "gz")

    left, right = call(rows_kernel, [shape(88, L), shape(88, L)], [sm, v, v, v])(
        gz_only, both, near_straight, near_cross
    )
    up = [(i, (i + 1) % gx_count) for i in range(gx_count)]
    down = [(j, i) for i, j in up]
    from_left = lax.ppermute(right, "gx", up)
    from_right = lax.ppermute(left, "gx", down)

    weights = call(
        weights_kernel,
        [
            shape(3, C, 96),
            shape(3, 64, 256),
            shape(3, C, 24),
            shape(3, 16, 256),
            shape(2, C, 1152),
            shape(2, 384, 384),
            shape(C, 16),
            shape(C, L),
            shape(4, L),
        ],
        [v] * 5,
        flops=10**7,
        vmem=8,
    )(species_embed, radial_weight, mix_weight, readout.reshape(1, C), energy_offset.reshape(1, 4))

    scratch = [
        VMEM((18, 8, L), f32),
        VMEM((8, 32, L), f32),
        VMEM((8, 18, E, L), f32),
        VMEM((8, E, NB, L), f32),
        VMEM((8, E, NB, L), f32),
        VMEM((8, 9, 64, L), f32),
        VMEM((4, 9, C, 2 * L), f32),
        VMEM((3, C, 2 * L), f32),
        VMEM((2, 768, L), f32),
        VMEM((8, C, L), f32),
        VMEM((4, C, 2 * L), f32),
        VMEM((4, C, 2 * L), f32),
        VMEM((8, 9, 32, L), f32),
        VMEM((18, E, L), f32),
        VMEM((E, 24, L), f32),
        VMEM((6, 256, L), bf16),
        VMEM((E, C, L), f32),
        VMEM((E, 3, C, L), f32),
        VMEM((9, C, L), f32),
        VMEM((1, 768, L), f32),
        VMEM((2, 256, L), f32),
        VMEM((2, 256, L), f32),
        VMEM((2, 3, 256, L), f32),
        VMEM((2, 3, 256, L), f32),
        VMEM((3, 256, 256), f32),
        VMEM((3, 2, E, 4, 8, L), f32),
        VMEM((9, 2, 256, L), f32),
        VMEM((18, 8, L), f32),
        VMEM((2, 8, L), f32),
    ]
    out_left, out_own, out_right = call(
        main_kernel, [shape(24, L)] * 3, [v] * 13, scratch, flops=10**9, vmem=48
    )(left, right, from_left, from_right, *weights)

    back_right = lax.ppermute(out_left, "gx", down)
    back_left = lax.ppermute(out_right, "gx", up)
    chunks = call(chunk_kernel, shape(gy_count * 2, 8, L), [sm, sm, v, v, v])(gy_only, gz_only, out_own, back_left, back_right)
    got = lax.all_to_all(chunks, yz, 0, 0)
    energy, force = call(unpack_kernel, [shape(32, 8), shape(96, 8)], [sm, v])(gy_only, got)
    return energy.reshape(2, 4, 4, 8), force.reshape(2, 4, 3, 4, 8).transpose(0, 1, 3, 4, 2)


def solution(mesh):
    in_specs = (
        P("gx", "gy", "gz", None, None),
        P("gx", "gy", "gz", None),
        P("gx", "gy", "gz", None, None),
        P("gx", "gy", "gz", None, None),
        P(),
        P(),
        P(),
        P(),
        P(),
    )
    out_specs = (P("gx", "gy", "gz", None), P("gx", "gy", "gz", None, None))
    return jax.shard_map(shards, mesh=mesh, in_specs=in_specs, out_specs=out_specs, check_vma=False)
```

```python
import math

import jax
import jax.numpy as jnp
from jax import lax
from jax.experimental import pallas as pl
from jax.experimental.pallas import tpu as pltpu
from jax.sharding import PartitionSpec as P


f32 = jnp.float32
bf16 = jnp.bfloat16
i32 = jnp.int32

E = 16
C = 128
NB = 8
L = 128
CUT = 2.0
GAMMA = ((NB - 1) / CUT) ** 2
SCALE = E**-0.5
PACK_VMEM = 4
R3 = math.sqrt(3.0)
R5 = math.sqrt(5.0)
R15 = math.sqrt(15.0)
VMEM = pltpu.VMEM
SMEM = pltpu.SMEM


def split2(x):
    return x, x - x.astype(bf16).astype(f32)


def split3(x):
    high = x.astype(bf16)
    rest = x - high.astype(f32)
    mid = rest.astype(bf16)
    low = (rest - mid.astype(f32)).astype(bf16)
    return high, mid, low


def dot(a, b, dims=((1,), (0,))):
    return lax.dot_general(a, b, (dims, ((), ())), preferred_element_type=f32)


def iota(shape, dim):
    return lax.broadcasted_iota(i32, shape, dim)


def roll(x, shift):
    return pltpu.roll(x, shift % x.shape[-1], x.ndim - 1)


def lanes(shape):
    return iota(shape, len(shape) - 1)


def block_masks(count):
    row, lane = iota((32 * count, 256), 0), iota((32 * count, 256), 1)
    keep = (lane // 32 == row // (4 * count)) & ((lane // 8) % 4 == row % 4)
    spread8 = jnp.where(iota((8, 256), 1) % 8 == iota((8, 256), 0), 1.0, 0.0).astype(bf16)
    return keep, spread8


def pack_kernel(
    gz_ref, pos_hbm, spec_hbm, nbr_hbm, mask_hbm, emb_hbm, rad_hbm, mix_hbm, read_hbm, off_hbm,
    own_ref, straight_ref, cross_ref, emb_ref, rad_ref, mix_ref, read_ref, off_ref,
    pos_ref, spec_ref, nbr_ref, mask_ref, sems,
):
    pairs = (
        (nbr_hbm, nbr_ref), (mask_hbm, mask_ref), (pos_hbm, pos_ref), (spec_hbm, spec_ref),
        (emb_hbm, emb_ref), (rad_hbm, rad_ref), (mix_hbm, mix_ref), (read_hbm, read_ref), (off_hbm, off_ref),
    )
    copies = [pltpu.make_async_copy(src, dst, sems.at[i]) for i, (src, dst) in enumerate(pairs)]
    for copy in copies:
        copy.start()
    for copy in copies[:4]:
        copy.wait()
    eye16 = jnp.where(iota((E, E), 0) == iota((E, E), 1), 1.0, 0.0).astype(bf16)
    own_ref[0:16, :] = dot(eye16, nbr_ref[...].astype(f32).astype(bf16), ((1,), (1,)))
    own_ref[16:32, :] = dot(eye16, mask_ref[...].astype(f32).astype(bf16), ((1,), (1,)))
    keep, spread8 = block_masks(3)
    group = jnp.where((iota((8, 96), 1) // 4) % 3 == iota((8, 96), 0), 1.0, 0.0).astype(bf16)
    tail = None
    for part in split3(pos_ref[...]):
        rows = jnp.where(keep, dot(part, spread8), 0.0).astype(bf16)
        piece = dot(group, rows)
        tail = piece if tail is None else tail + piece
    keep, _ = block_masks(1)
    kinds = jnp.where(keep, dot(spec_ref[...].astype(f32).astype(bf16), spread8), 0.0)
    species = jnp.sum(kinds, 0, keepdims=True)
    own_ref[32:40, :] = jnp.where(iota((8, 256), 0) == 3, species, tail)

    lower = lanes((40, L)) < 64
    first, second = own_ref[:, 0:128], own_ref[:, 128:256]
    rows_low = jnp.where(lower, first, roll(second, 64))
    rows_high = jnp.where(lower, roll(first, 64), second)
    front = gz_ref[0] == 0
    straight_ref[...] = jnp.where(front, rows_high, rows_low)
    cross_ref[...] = jnp.where(front, rows_low, rows_high)
    for copy in copies[4:]:
        copy.wait()


def spread(half0, half1, start):
    quarter = lanes((40, L)) // 32
    out = roll(half0, -start)
    out = jnp.where(quarter == 1, roll(half1, 32 - start), out)
    out = jnp.where(quarter == 2, roll(half0, 32 - start), out)
    return jnp.where(quarter == 3, roll(half1, 64 - start), out)


def halves(first, second):
    return roll(jnp.where(lanes(first.shape) >= 64, first, second), 64)


def rows_kernel(gz_ref, other_ref, own_ref, straight_ref, cross_ref, left_ref, right_ref):
    front = gz_ref[0] == 0
    all_ref = [jnp.where(front, own_ref[...], other_ref[...]), jnp.where(front, other_ref[...], own_ref[...])]
    near0 = jnp.where(front, straight_ref[...], cross_ref[...])
    near1 = jnp.where(front, cross_ref[...], straight_ref[...])
    for x in range(2):
        near = spread(near0, near1, 64 * x)
        own = [
            spread(all_ref[0][:, x * L : (x + 1) * L], all_ref[1][:, x * L : (x + 1) * L], 64 * pair)
            for pair in range(2)
        ]
        tiles = [
            jnp.where(front, near, own[0]),
            jnp.where(front, own[0], own[1]),
            jnp.where(front, own[1], near),
        ]
        for pair in range(3):
            at = (x * 3 + pair) * 4
            left_ref[at : at + 4, :] = tiles[pair][32:36]
            right_ref[at : at + 4, :] = tiles[pair][32:36]
        out = left_ref if x == 0 else right_ref
        for r in range(2):
            out[24 + 32 * r : 56 + 32 * r, :] = halves(tiles[r][0:32], tiles[r + 1][0:32])


def weights_kernel(
    emb_ref, rad_ref, mix_ref, read_ref, off_ref, vf_ref, vb_ref, wf_ref, wb_ref, mf_ref, mb_ref, et_ref, ro_ref, eo_ref
):
    emb = emb_ref[...]
    for q in range(3):
        base = rad_ref[0, :, q * C : (q + 1) * C] * SCALE
        v = jnp.concatenate([base * emb[k : k + 1] for k in range(4)], 0)
        high, low = split2(v)
        vb_ref[q, 0:32, 0:128] = high
        vb_ref[q, 0:32, 128:256] = high
        vb_ref[q, 32:64, 0:128] = low
        vb_ref[q, 32:64, 128:256] = jnp.zeros((32, 128), f32)
        high, low = split2(v.T)
        vf_ref[q] = jnp.concatenate([high, high, low], 1)
        w = rad_ref[1, :, q * C : (q + 1) * C]
        both = jnp.concatenate(split2(w), 0)
        wb_ref[q, :, 0:128] = both
        wb_ref[q, :, 128:256] = jnp.where(iota((16, 128), 0) < 8, both, 0.0)
        high, low = split2(w.T)
        wf_ref[q] = jnp.concatenate([high, high, low], 1)
    for layer in range(2):
        for q in range(3):
            m = mix_ref[layer, q * C : (q + 1) * C, :]
            high, low = split2(m)
            mb_ref[layer, q * C : (q + 1) * C, 0:128] = high
            mb_ref[layer, q * C : (q + 1) * C, 128:256] = high
            mb_ref[layer, q * C : (q + 1) * C, 256:384] = low
            high, low = split2(m.T)
            mf_ref[layer, :, q * C : (q + 1) * C] = high
            mf_ref[layer, :, 384 + q * C : 384 + (q + 1) * C] = high
            mf_ref[layer, :, 768 + q * C : 768 + (q + 1) * C] = low
    high, mid, low = split3(emb)
    stack = jnp.concatenate([high.astype(f32), mid.astype(f32), low.astype(f32), jnp.zeros((4, C), f32)], 0)
    et_ref[...] = stack.T
    ro_ref[...] = jnp.broadcast_to(read_ref[...], (C, L)).T
    pick = jnp.where(iota((4, 4), 0) == iota((4, 4), 1), off_ref[...], 0.0)
    eo_ref[...] = jnp.broadcast_to(jnp.sum(pick, 1, keepdims=True), (4, L))


def decode(ids):
    cell = ids >> 3
    ox = (cell >= 9).astype(i32) + (cell >= 18).astype(i32)
    rest = cell - 9 * ox
    oy = (rest >= 3).astype(i32) + (rest >= 6).astype(i32)
    oz = rest - 3 * oy
    lane = lanes(ids.shape)
    ys = (lane >> 6) + oy
    zs = ((lane >> 3) + oz + 7) & 7
    tile = ox * 2 + (ys >> 1)
    target = ((ys & 1) << 6) | (zs << 3) | (ids & 7)
    return ox, oy, oz, tile, target


PX, PY, PZ, RAD, RINV, UM, TM, SP, TILE, TARGET, Y1X, Y1Y, Y1Z, Y20, Y21, Y22, Y23, Y24 = range(18)
COUNTS = (1, 3, 5)
HALF = (1.0,) + (0.5 * R3,) * 3 + (0.5 * R15, 0.5 * R15, 0.5 * R5, 0.5 * R15, 0.5 * R15)


def silu_parts(v):
    gate = 1.0 / (1.0 + jnp.exp(-v))
    return v * gate, gate * (1.0 + v * (1.0 - gate))


def order_of(qm):
    return 0 if qm == 0 else 1 if qm < 4 else 2


def one_hot_block(code16, block):
    spot = (iota((16, L), 0) + 16 * block).astype(f32).astype(bf16)
    return jnp.where(spot == code16, jnp.ones((), bf16), jnp.zeros((), bf16))


def main_kernel(
    lown_ref, rown_ref, froml_ref, fromr_ref,
    vf_ref, vb_ref, wf_ref, wb_ref, mf_ref, mb_ref, et_ref, ro_ref, eo_ref,
    outl_ref, outo_ref, outr_ref,
    table, edges, geo, basis, slope, psplit, moment, zbuf, inv, hid, dsilu, dhid, dmom, geo2,
    rbst, hg, hs, rad2, efac, invx, dha, dhb, dra, drb, dacc, extra, dsplit, force, energy,
):
    for plane, (ref, base) in enumerate(
        ((froml_ref, 0), (froml_ref, 1), (lown_ref, 0), (lown_ref, 1), (fromr_ref, 0), (fromr_ref, 1))
    ):
        for pair in range(3):
            at = (base * 3 + pair) * 4
            table[plane * 3 + pair, 0:4, :] = ref[at : at + 4, :]
    for plane, ref in enumerate((froml_ref, lown_ref, rown_ref, fromr_ref)):
        for r in range(2):
            edges[plane * 2 + r] = ref[24 + 32 * r : 56 + 32 * r, :]

    centre = iota((NB, L), 0).astype(f32) * (CUT / (NB - 1))

    def sums(xr, r):
        at = xr * 2 + r
        base = (xr + 1) * 3 + r
        own = halves(table[base], table[base + 1])
        ids = edges[at, 0:16, :].astype(i32)
        ox, oy, oz, tile, target = decode(ids)
        got = [jnp.zeros((E, L), f32) for _ in range(4)]
        for t in range(6):
            src = table[(xr + t // 2) * 3 + r + t % 2]
            here = tile == t
            for q in range(4):
                wide = jnp.broadcast_to(src[q : q + 1], (E, L))
                val = jnp.take_along_axis(wide, target, axis=1, mode="promise_in_bounds")
                got[q] = jnp.where(here, val, got[q])
        dx = ((ox - 1).astype(f32) + got[0]) - own[0:1]
        dy = ((oy - 1).astype(f32) + got[1]) - own[1:2]
        dz = ((oz - 1).astype(f32) + got[2]) - own[2:3]
        sq = dx * dx + dy * dy + dz * dz
        dist = jnp.sqrt(sq)
        part = jnp.where(dist < CUT, 1.0 - sq * (1.0 / CUT**2), 0.0) * edges[at, 16:32, :]
        px, py, pz = 0.5 * dx, 0.5 * dy, 0.5 * dz
        geo[at, PX] = px
        geo[at, PY] = py
        geo[at, PZ] = pz
        geo[at, RAD] = dist
        geo[at, RINV] = lax.rsqrt(sq)
        geo[at, UM] = part * part
        geo[at, TM] = part
        geo[at, SP] = got[3]
        geo[at, TILE] = tile.astype(f32)
        geo[at, TARGET] = target.astype(f32)
        geo[at, Y1X] = R3 * px
        geo[at, Y1Y] = R3 * py
        geo[at, Y1Z] = R3 * pz
        geo[at, Y20] = R15 * px * py
        geo[at, Y21] = R15 * py * pz
        geo[at, Y22] = (0.5 * R5) * (2.0 * pz * pz - px * px - py * py)
        geo[at, Y23] = R15 * px * pz
        geo[at, Y24] = (0.5 * R15) * (px * px - py * py)

        def row(i, e):
            return jnp.broadcast_to(geo[at, i, e : e + 1, :], (NB, L))

        for e in range(E):
            diff = row(RAD, e) - centre
            bump = jnp.exp(-GAMMA * (diff * diff))
            rb = bump * row(UM, e)
            basis[at, e] = rb
            slope[at, e] = (-2.0) * (bump * row(TM, e)) - (4.0 * GAMMA) * (diff * rb * row(RINV, e))
        acc = [[None] * 4 for _ in range(9)]
        for e in range(E):
            rb = basis[at, e]
            kind = row(SP, e)
            per = [jnp.where(kind == float(k), rb, 0.0) for k in range(4)]
            for qm in range(9):
                y = None if qm == 0 else row(Y1X + qm - 1, e)
                for k in range(4):
                    term = per[k] if y is None else y * per[k]
                    acc[qm][k] = term if e == 0 else acc[qm][k] + term
        for qm in range(9):
            for k in range(4):
                high, low = split2(acc[qm][k])
                psplit[at, qm, k * 8 : k * 8 + 8] = high
                psplit[at, qm, 32 + k * 8 : 40 + k * 8] = low

    def invariants(source, dest, width):
        for i in range(8):
            rows = slice(i * 16, i * 16 + 16)
            first = 0
            for q, count in enumerate(COUNTS):
                value = source(first, rows)
                if q > 0:
                    value = value * value
                    for m in range(1, count):
                        a = source(first + m, rows)
                        value = value + a * a
                first += count
                for r in range(width):
                    high, low = split2(value[:, r * L : (r + 1) * L])
                    dest[r, q * C + i * 16 : q * C + i * 16 + 16] = high
                    dest[r, 384 + q * C + i * 16 : 384 + q * C + i * 16 + 16] = low

    def features(xr):
        for qm in range(9):
            both = jnp.concatenate([psplit[xr * 2, qm], psplit[xr * 2 + 1, qm]], 1)
            moment[xr, qm] = dot(vf_ref[order_of(qm)], jnp.concatenate([both, both[0:32]], 0))
        invariants(lambda qm, rows: moment[xr, qm, rows, :], inv, 2)
        both = jnp.concatenate([inv[0], inv[1]], 1)
        zbuf[0] = dot(mf_ref[0], jnp.concatenate([both, both[0:384]], 0))
        sel = iota((16, L), 0)
        hots = []
        for r in range(2):
            base = (xr + 1) * 3 + r
            own = halves(table[base], table[base + 1])
            kind = jnp.broadcast_to(own[3:4], (16, L))
            hots.append(jnp.where((kind == (sel % 4).astype(f32)) & (sel < 12), 1.0, 0.0))
        zbuf[1] = dot(et_ref[...], jnp.concatenate(hots, 1))
        for i in range(16):
            rows = slice(i * 8, i * 8 + 8)
            update, slope_z = silu_parts(zbuf[0, rows, :])
            h1 = zbuf[1, rows, :] + update
            hid[xr * 2, rows, :] = h1[:, 0:L]
            hid[xr * 2 + 1, rows, :] = h1[:, L:]
            dsilu[xr, rows, :] = slope_z

    def layer_one(xr, _):
        features(xr)
        sums(xr + 1, 0)
        sums(xr + 1, 1)
        return 0

    sums(0, 0)
    sums(0, 1)
    lax.fori_loop(0, 3, layer_one, 0)
    features(3)

    low_half = lanes((C, L)) < 64
    for plane in range(4):
        for r in range(2):
            if plane in (1, 2):
                keep = low_half if r == 1 else ~low_half
                dhid[plane, :, r * L : (r + 1) * L] = jnp.where(keep, ro_ref[...], 0.0)
            else:
                dhid[plane, :, r * L : (r + 1) * L] = jnp.zeros((C, L), f32)
    for r in range(2):
        for e in range(E):
            for i in range(4):
                extra[0, r, e, i] = jnp.zeros((8, L), f32)
    lane8 = lanes((8, L))

    def layer_two(x, _):
        a, b = (x + 1) * 2, (x + 1) * 2 + 1
        ids = halves(edges[a, 0:16, :], edges[b, 0:16, :]).astype(i32)
        _, _, _, tile, target = decode(ids)
        geo2[TILE] = tile.astype(f32)
        geo2[TARGET] = target.astype(f32)
        for i in (PX, PY, PZ, Y1X, Y1Y, Y1Z, Y20, Y21, Y22, Y23, Y24):
            geo2[i] = halves(geo[a, i], geo[b, i])
        for e in range(E):
            rb = halves(basis[a, e], basis[b, e])
            high, low = split2(rb)
            rbst[e] = jnp.concatenate([high, low, high], 0)

        for t in range(6):
            high, low = split2(hid[(x + t // 2) * 2 + t % 2])
            hg[t, 0:128] = high.astype(bf16)
            hg[t, 128:256] = low.astype(bf16)

        def code_row(i, e):
            return jnp.broadcast_to(geo2[i, pl.ds(e, 1), :], (16, L))

        def hot_blocks(pair, which):
            tiles = [code_row(TILE, 2 * pair + half) for half in range(2)]
            spots = [code_row(TARGET, 2 * pair + half) for half in range(2)]
            blocks = []
            for t in which:
                codes = [jnp.where(tiles[i] == float(t), spots[i], -1.0).astype(bf16) for i in range(2)]
                for block in range(8):
                    blocks.append(jnp.concatenate([one_hot_block(code, block) for code in codes], 1))
            return jnp.concatenate(blocks, 0)

        def gather(pair):
            table_x = jnp.concatenate([hg[t] for t in range(6)], 1)
            out = dot(table_x, hot_blocks(pair, range(6)))
            both = jnp.concatenate([rbst[2 * pair], rbst[2 * pair + 1]], 1)
            for half in range(2):
                cols = slice(half * L, (half + 1) * L)
                hs[2 * pair + half] = out[0:128, cols] + out[128:256, cols]
            for q in range(3):
                rad = dot(wf_ref[q], both)
                rad2[2 * pair, q] = rad[:, 0:L]
                rad2[2 * pair + 1, q] = rad[:, L:]

        def contract(pair):
            for i in range(8):
                rows = slice(i * 16, i * 16 + 16)
                acc = [None if pair == 0 else efac[qm, rows, :] for qm in range(9)]
                for e in (2 * pair, 2 * pair + 1):
                    h = hs[e, rows, :]
                    ts = [rad2[e, q, rows, :] * h for q in range(3)]
                    for qm in range(9):
                        if qm == 0:
                            term = ts[0]
                        else:
                            y = jnp.broadcast_to(geo2[Y1X + qm - 1, e : e + 1, :], (16, L))
                            term = y * ts[order_of(qm)]
                        acc[qm] = term if acc[qm] is None else acc[qm] + term
                for qm in range(9):
                    efac[qm, rows, :] = acc[qm] * SCALE if pair == 7 else acc[qm]

        gather(0)
        for pair in range(8):
            if pair < 7:
                gather(pair + 1)
            contract(pair)

        invariants(lambda qm, rows: efac[qm, rows, :], invx, 1)
        zbuf[0, :, 0:L] = dot(mf_ref[1], jnp.concatenate([invx[0], invx[0, 0:384]], 0))
        total = jnp.zeros((8, L), f32)
        for i in range(8):
            rows = slice(i * 16, i * 16 + 16)
            update, slope_z = silu_parts(zbuf[0, rows, 0:L])
            term = ro_ref[rows, :] * (halves(hid[a, rows, :], hid[b, rows, :]) + update)
            total = total + (term[0:8] + term[8:16])
            high, low = split2(ro_ref[rows, :] * slope_z)
            invx[0, i * 16 : i * 16 + 16] = high
            invx[0, 128 + i * 16 : 144 + i * 16] = low
        kind = table[(x + 2) * 3 + 1, 3:4, :]
        offset = jnp.zeros((1, L), f32)
        for k in range(4):
            offset = jnp.where(kind == float(k), eo_ref[k : k + 1, :], offset)
        energy[x] = jnp.broadcast_to(jnp.sum(total, 0, keepdims=True) + offset, (8, L))

        both = jnp.concatenate([invx[0, 0:256], invx[0, 0:128]], 0)
        zbuf[0, :, 0:L] = dot(mb_ref[1, 0:128], both)
        zbuf[0, :, L:] = dot(mb_ref[1, 128:256], both)
        zbuf[1, :, 0:L] = dot(mb_ref[1, 256:384], both)
        for i in range(8):
            rows = slice(i * 16, i * 16 + 16)
            efac[0, rows, :] = zbuf[0, rows, 0:L] * SCALE
            one = zbuf[0, rows, L:] * (2.0 * SCALE)
            two = zbuf[1, rows, 0:L] * (2.0 * SCALE)
            for m in range(1, 9):
                efac[m, rows, :] = efac[m, rows, :] * (one if m < 4 else two)

        def edge_grad(e, dh, dr):
            def row(i, n):
                return jnp.broadcast_to(geo2[i, pl.ds(e, 1), :], (n, L))

            ys = [None] + [row(Y1X + m, 16) for m in range(8)]
            acc = [None] * 9
            for i in range(8):
                rows = slice(i * 16, i * 16 + 16)
                low_rows = slice(128 + i * 16, 144 + i * 16)
                h = hs[e, rows, :]
                rr = [rad2[e, q, rows, :] for q in range(3)]
                ef = [efac[qm, rows, :] for qm in range(9)]
                d0 = ef[0]
                d1 = ys[1] * ef[1] + ys[2] * ef[2] + ys[3] * ef[3]
                d2 = ys[4] * ef[4] + ys[5] * ef[5] + ys[6] * ef[6] + ys[7] * ef[7] + ys[8] * ef[8]
                t1 = rr[1] * h
                t2 = rr[2] * h
                for qm in range(1, 9):
                    term = (t1 if qm < 4 else t2) * ef[qm]
                    term = term[0:8] + term[8:16]
                    acc[qm] = term if i == 0 else acc[qm] + term
                dh[rows], dh[low_rows] = split2(d0 * rr[0] + d1 * rr[1] + d2 * rr[2])
                for q, d in enumerate((d0, d1, d2)):
                    dr[q, rows], dr[q, low_rows] = split2(d * h)
            px, py, pz = (row(i, 8) for i in (PX, PY, PZ))
            gx = R3 * acc[1] + R15 * (py * acc[4] + pz * acc[7] + px * acc[8]) - R5 * (px * acc[6])
            gy = R3 * acc[2] + R15 * (px * acc[4] + pz * acc[5] - py * acc[8]) - R5 * (py * acc[6])
            gz = R3 * acc[3] + R15 * (py * acc[5] + px * acc[7]) + (2.0 * R5) * (pz * acc[6])
            for i, g in enumerate((gx, gy, gz)):
                turned = roll(0.5 * g, 64)
                extra[x + 1, 0, e, i + 1] = jnp.where(lane8 >= 64, turned, 0.0)
                extra[x + 1, 1, e, i + 1] = jnp.where(lane8 < 64, turned, 0.0)

        def spread_back(pair, dh, dr):
            grad = None
            for q in range(3):
                piece = dot(wb_ref[q], jnp.concatenate([dr[0, q], dr[1, q]], 1))
                grad = piece if grad is None else grad + piece
            grad = grad[0:8] + grad[8:16]
            for half in range(2):
                turned = roll(grad[:, half * L : (half + 1) * L], 64)
                extra[x + 1, 0, 2 * pair + half, 0] = jnp.where(lane8 >= 64, turned, 0.0)
                extra[x + 1, 1, 2 * pair + half, 0] = jnp.where(lane8 < 64, turned, 0.0)
            left = jnp.concatenate([dh[0], dh[1]], 1).astype(bf16)

            for part in range(3):
                hot = hot_blocks(pair, (2 * part, 2 * part + 1))
                dacc[part] = dacc[part] + dot(left, hot, ((1,), (1,)))

        for part in range(3):
            dacc[part] = jnp.zeros((256, 256), f32)
        for half in range(2):
            edge_grad(half, dhb.at[half], drb.at[half])

        def back(i, _):
            for half in range(2):
                edge_grad(4 * i + 2 + half, dha.at[half], dra.at[half])
            spread_back(2 * i, dhb, drb)
            for half in range(2):
                edge_grad(4 * i + 4 + half, dhb.at[half], drb.at[half])
            spread_back(2 * i + 1, dha, dra)
            return 0

        lax.fori_loop(0, 3, back, 0)
        for half in range(2):
            edge_grad(14 + half, dha.at[half], dra.at[half])
        spread_back(6, dhb, drb)
        spread_back(7, dha, dra)
        for part in range(3):
            for i in range(8):
                rows = slice(i * 16, i * 16 + 16)
                total = dacc[part, rows, :] + dacc[part, 128 + i * 16 : 144 + i * 16, :]
                dhid[x + part, rows, :] = dhid[x + part, rows, :] + total
        return 0

    lax.fori_loop(0, 2, layer_two, 0)

    def sums_back(xr):
        for i in range(8):
            rows = slice(i * 16, i * 16 + 16)
            value = dhid[xr, rows, :] * dsilu[xr, rows, :]
            for r in range(2):
                high, low = split2(value[:, r * L : (r + 1) * L])
                inv[r, i * 16 : i * 16 + 16] = high
                inv[r, 128 + i * 16 : 144 + i * 16] = low
        both = jnp.concatenate([inv[0, 0:256], inv[1, 0:256]], 1)
        both = jnp.concatenate([both, both[0:128]], 0)
        for q in range(3):
            zbuf[q] = dot(mb_ref[0, q * C : (q + 1) * C], both)
        for i in range(8):
            rows = slice(i * 16, i * 16 + 16)
            parts = [zbuf[0, rows, :], 2.0 * zbuf[1, rows, :], 2.0 * zbuf[2, rows, :]]
            for qm in range(9):
                value = parts[0] if qm == 0 else parts[order_of(qm)] * moment[xr, qm, rows, :]
                for r in range(2):
                    high, low = split2(value[:, r * L : (r + 1) * L])
                    dsplit[qm, r, i * 16 : i * 16 + 16] = high
                    dsplit[qm, r, 128 + i * 16 : 144 + i * 16] = low
        for qm in range(9):
            out = dot(vb_ref[order_of(qm)], jnp.concatenate([dsplit[qm, 0], dsplit[qm, 1]], 1))
            out = HALF[qm] * (out[0:32] + out[32:64])
            dmom[xr * 2, qm] = out[:, 0:L]
            dmom[xr * 2 + 1, qm] = out[:, L:]

    for i in range(18):
        force[i] = jnp.zeros((8, L), f32)
    sub8 = iota((8, L), 0)

    def forces(xr):
        slab = xr % 3 if isinstance(xr, int) else jnp.where((xr == 1) | (xr == 2), xr, 0)
        for r in range(2):
            at = xr * 2 + r
            received = jnp.zeros((8, L), f32)
            picks, hots = [], []
            for e in range(E):
                def row(i):
                    return jnp.broadcast_to(geo[at, i, e : e + 1, :], (NB, L))

                kind = row(SP)
                is0, is1, is2 = kind == 0.0, kind == 1.0, kind == 2.0
                dp = []
                for qm in range(9):
                    sel = jnp.where(is2, dmom[at, qm, 16:24, :], dmom[at, qm, 24:32, :])
                    sel = jnp.where(is1, dmom[at, qm, 8:16, :], sel)
                    dp.append(jnp.where(is0, dmom[at, qm, 0:8, :], sel))
                px, py, pz = row(PX), row(PY), row(PZ)
                dz6 = dp[6] * pz
                gx = dp[1] + py * dp[4] + pz * dp[7] + px * (dp[8] - dp[6])
                gy = dp[2] + px * dp[4] + pz * dp[5] - py * (dp[8] + dp[6])
                gz = dp[3] + py * dp[5] + px * dp[7] + (dz6 + dz6)
                g = dp[0] + px * (gx + dp[1]) + py * (gy + dp[2]) + pz * (gz + dp[3])
                g = g + extra[slab, r, e, 0]
                radial = g * slope[at, e]
                rb = basis[at, e]
                gx = px * radial + rb * gx + extra[slab, r, e, 1]
                gy = py * radial + rb * gy + extra[slab, r, e, 2]
                gz = pz * radial + rb * gz + extra[slab, r, e, 3]
                sx = jnp.sum(gx, 0, keepdims=True)
                sy = jnp.sum(gy, 0, keepdims=True)
                sz = jnp.sum(gz, 0, keepdims=True)
                vec = jnp.where(sub8 == 0, sx, jnp.where(sub8 == 1, sy, jnp.where(sub8 == 2, sz, 0.0)))
                received = received + vec
                both = jnp.concatenate(split2(vec), 0).astype(bf16)
                where_t = jnp.broadcast_to(geo[at, TILE, e : e + 1, :], (16, L)).astype(bf16)
                picks.append(
                    [jnp.where(where_t == jnp.full((), t, bf16), both, jnp.zeros((), bf16)) for t in range(6)]
                )
                code = jnp.broadcast_to(geo[at, TARGET, e : e + 1, :], (16, L)).astype(bf16)
                hots.append([one_hot_block(code, block) for block in range(8)])
                if e % 2:
                    left = jnp.concatenate([jnp.concatenate(p, 0) for p in picks], 1)
                    right = jnp.concatenate([jnp.concatenate(h, 0) for h in hots], 1)
                    piece = dot(left, right, ((1,), (1,)))
                    sent = piece if e == 1 else sent + piece
                    picks, hots = [], []
            for t in range(6):
                to = (xr + t // 2) * 3 + r + t % 2
                force[to] = force[to] - (sent[t * 16 : t * 16 + 8] + sent[t * 16 + 8 : t * 16 + 16])
            turned = roll(received, 64)
            mine = (xr + 1) * 3 + r
            force[mine] = force[mine] + jnp.where(lane8 >= 64, turned, 0.0)
            force[mine + 1] = force[mine + 1] + jnp.where(lane8 < 64, turned, 0.0)

    def layer_one_back(xr, _):
        sums_back(xr + 1)
        forces(xr)
        return 0

    sums_back(0)
    lax.fori_loop(0, 3, layer_one_back, 0)
    forces(3)

    for plane in range(6):
        for pair in range(3):
            out = (outl_ref, outo_ref, outr_ref)[plane // 2]
            at = ((plane % 2) * 3 + pair) * 4
            out[at : at + 4, :] = force[plane * 3 + pair, 0:4, :]
            if plane in (2, 3) and pair == 1:
                out[at + 3 : at + 4, :] = energy[plane - 2, 0:1, :]


def chunk_kernel(gy_ref, gz_ref, own_ref, left_ref, right_ref, out_ref):
    gy, gz = gy_ref[0], gz_ref[0]
    front = gz == 0
    total = own_ref[...] + left_ref[...] + right_ref[...]
    quarter = lanes((4, L)) // 32

    def squeeze(pair, zh):
        first = total[pair * 4 : pair * 4 + 4]
        second = total[12 + pair * 4 : 16 + pair * 4]
        out = roll(first, -32 * zh)
        out = jnp.where(quarter == 1, roll(first, -32 - 32 * zh), out)
        out = jnp.where(quarter == 2, roll(second, 64 - 32 * zh), out)
        return jnp.where(quarter == 3, roll(second, 32 - 32 * zh), out)

    out_ref[...] = jnp.zeros(out_ref.shape, f32)
    y_count = out_ref.shape[0] // 2
    beside = jnp.where(front, gy + y_count - 1, gy + 1)
    beside = jnp.where(beside >= y_count, beside - y_count, beside)
    for zh in range(2):
        parts = [squeeze(pair, zh) for pair in range(3)]
        low = jnp.where(front, parts[1], parts[0])
        high = jnp.where(front, parts[2], parts[1])
        near = jnp.where(front, parts[0], parts[2])
        out_ref[gy * 2 + zh] = jnp.concatenate([low, high], 0)
        out_ref[beside * 2 + zh, 0:4, :] = near


def unpack_kernel(gy_ref, got_ref, energy_ref, force_ref):
    gy = gy_ref[0]
    y_count = got_ref.shape[0] // 2
    below = jnp.where(gy == 0, y_count - 1, gy - 1)
    above = jnp.where(gy == y_count - 1, 0, gy + 1)
    own = got_ref[gy * 2] + got_ref[gy * 2 + 1]
    low = own[0:4] + got_ref[below * 2 + 1, 0:4, :]
    high = own[4:8] + got_ref[above * 2, 0:4, :]
    lower = lanes((4, L)) < 64
    first = jnp.where(lower, low, roll(high, 64))
    second = jnp.where(lower, roll(low, 64), high)
    rows = jnp.concatenate([first, second], 1)
    keep, spread8 = block_masks(3)
    group = jnp.where((iota((96, 8), 0) // 4) % 3 == iota((96, 8), 1), 1.0, 0.0).astype(bf16)
    rows8 = jnp.concatenate([rows, jnp.zeros((4, 256), f32)], 0)
    nt = ((1,), (1,))
    total = None
    for part in split3(rows8):
        wide = jnp.where(keep, dot(group, part), 0.0).astype(bf16)
        piece = dot(wide, spread8, nt)
        total = piece if total is None else total + piece
    force_ref[...] = total
    keep, _ = block_masks(1)
    total = None
    for part in split3(rows[3:4]):
        wide = jnp.where(keep, part.astype(f32), 0.0).astype(bf16)
        piece = dot(wide, spread8, nt)
        total = piece if total is None else total + piece
    energy_ref[...] = total


def call(kernel, outs, in_specs, scratch=(), flops=10**6, vmem=4):
    return pl.pallas_call(
        kernel,
        out_shape=outs,
        in_specs=in_specs,
        out_specs=jax.tree.map(lambda _: pl.BlockSpec(memory_space=VMEM), outs),
        scratch_shapes=list(scratch),
        compiler_params=pltpu.CompilerParams(vmem_limit_bytes=int(vmem * 2**20)),
        cost_estimate=pl.CostEstimate(flops=flops, bytes_accessed=10**5, transcendentals=0),
    )


def shape(*dims, dtype=f32):
    return jax.ShapeDtypeStruct(dims, dtype)


def shards(
    positions, species, neighbors, edge_mask, species_embed, radial_weight, mix_weight, readout, energy_offset
):
    v = pl.BlockSpec(memory_space=VMEM)
    sm = pl.BlockSpec(memory_space=SMEM)
    gy_count, gz_count = lax.axis_size("gy"), lax.axis_size("gz")
    gx_count = lax.axis_size("gx")
    gy, gz = lax.axis_index("gy"), lax.axis_index("gz")
    gy_only = gy.astype(i32).reshape(1)
    gz_only = gz.astype(i32).reshape(1)

    own, straight, cross, *raw = call(
        pack_kernel,
        [shape(40, 256), shape(40, L), shape(40, L)]
        + [shape(4, C), shape(2, NB, 384), shape(2, 384, C), shape(1, C), shape(1, 4)],
        [sm] + [pl.BlockSpec(memory_space=pltpu.HBM)] * 9,
        [VMEM((96, 8), f32), VMEM((32, 8), i32), VMEM((256, E), i32), VMEM((256, E), i32), pltpu.SemaphoreType.DMA((9,))],
        vmem=PACK_VMEM,
    )(
        gz_only,
        *(
            pltpu.with_memory_space_constraint(x, pltpu.HBM)
            for x in (
                positions.transpose(0, 1, 4, 2, 3).reshape(96, 8),
                species.reshape(32, 8),
                neighbors.reshape(256, E),
                edge_mask.reshape(256, E),
                species_embed,
                radial_weight,
                mix_weight,
                readout.reshape(1, C),
                energy_offset.reshape(1, 4),
            )
        ),
    )

    def dev(y, s):
        return (y % gy_count) * gz_count + s

    yz = ("gy", "gz")
    go_straight = [(dev(y, s), dev(y + 1 if s == 0 else y - 1, s)) for y in range(gy_count) for s in range(2)]
    go_cross = [(dev(y, s), dev(y - 1 if s == 0 else y + 1, 1 - s)) for y in range(gy_count) for s in range(2)]
    near_straight = lax.ppermute(straight, yz, go_straight)
    near_cross = lax.ppermute(cross, yz, go_cross)
    both = lax.ppermute(own, "gz", [(0, 1), (1, 0)])

    left, right = call(rows_kernel, [shape(88, L), shape(88, L)], [sm, v, v, v, v])(
        gz_only, both, own, near_straight, near_cross
    )
    up = [(i, (i + 1) % gx_count) for i in range(gx_count)]
    down = [(j, i) for i, j in up]
    from_left = lax.ppermute(right, "gx", up)
    from_right = lax.ppermute(left, "gx", down)

    weights = call(
        weights_kernel,
        [
            shape(3, C, 96),
            shape(3, 64, 256),
            shape(3, C, 24),
            shape(3, 16, 256),
            shape(2, C, 1152),
            shape(2, 384, 384),
            shape(C, 16),
            shape(C, L),
            shape(4, L),
        ],
        [v] * 5,
        flops=10**7,
        vmem=8,
    )(*raw)

    scratch = [
        VMEM((18, 8, L), f32),
        VMEM((8, 32, L), f32),
        VMEM((8, 18, E, L), f32),
        VMEM((8, E, NB, L), f32),
        VMEM((8, E, NB, L), f32),
        VMEM((8, 9, 64, L), f32),
        VMEM((4, 9, C, 2 * L), f32),
        VMEM((3, C, 2 * L), f32),
        VMEM((2, 768, L), f32),
        VMEM((8, C, L), f32),
        VMEM((4, C, 2 * L), f32),
        VMEM((4, C, 2 * L), f32),
        VMEM((8, 9, 32, L), f32),
        VMEM((18, E, L), f32),
        VMEM((E, 24, L), f32),
        VMEM((6, 256, L), bf16),
        VMEM((E, C, L), f32),
        VMEM((E, 3, C, L), f32),
        VMEM((9, C, L), f32),
        VMEM((1, 768, L), f32),
        VMEM((2, 256, L), f32),
        VMEM((2, 256, L), f32),
        VMEM((2, 3, 256, L), f32),
        VMEM((2, 3, 256, L), f32),
        VMEM((3, 256, 256), f32),
        VMEM((3, 2, E, 4, 8, L), f32),
        VMEM((9, 2, 256, L), f32),
        VMEM((18, 8, L), f32),
        VMEM((2, 8, L), f32),
    ]
    out_left, out_own, out_right = call(
        main_kernel, [shape(24, L)] * 3, [v] * 13, scratch, flops=10**9, vmem=48
    )(left, right, from_left, from_right, *weights)

    back_right = lax.ppermute(out_left, "gx", down)
    back_left = lax.ppermute(out_right, "gx", up)
    chunks = call(chunk_kernel, shape(gy_count * 2, 8, L), [sm, sm, v, v, v])(gy_only, gz_only, out_own, back_left, back_right)
    got = lax.all_to_all(chunks, yz, 0, 0)
    energy, force = call(unpack_kernel, [shape(32, 8), shape(96, 8)], [sm, v])(gy_only, got)
    return energy.reshape(2, 4, 4, 8), force.reshape(2, 4, 3, 4, 8).transpose(0, 1, 3, 4, 2)


def solution(mesh):
    in_specs = (
        P("gx", "gy", "gz", None, None),
        P("gx", "gy", "gz", None),
        P("gx", "gy", "gz", None, None),
        P("gx", "gy", "gz", None, None),
        P(),
        P(),
        P(),
        P(),
        P(),
    )
    out_specs = (P("gx", "gy", "gz", None), P("gx", "gy", "gz", None, None))
    return jax.shard_map(shards, mesh=mesh, in_specs=in_specs, out_specs=out_specs, check_vma=False)
```
